32 devices in a mesh: seq: 8 (over z, core), fsdp: 4 (over y, x).
Axes of the slice: x: 2, y: 2, z: 4, core: 2. Of those that a mesh axis runs over, the one named last changes fastest.
Arguments:
- tokens: bfloat16 [4, 2048, 1536], P('fsdp', 'seq'), may hold values from -6 to 6
- seg_ids: int32 [4, 2048], P('fsdp'), may hold values from 0 to 3, never falling along the last dimension, each value on 1 to 1024 neighbouring positions
- pre_gain: float32 [1536], replicated, may hold values from 0.25 to 1.75
- w_in: bfloat16 [1536, 6448], P('fsdp'), may hold values from -0.15625 to 0.15625
- conv_weight: float32 [4, 3328], replicated, may hold values from -3 to 3
- conv_bias: float32 [3328], replicated, may hold values from -3 to 3
- dt_bias: float32 [48], replicated, may hold values from -6 to -2
- a_log: float32 [48], replicated, may hold values from -5 to 1.5
- d_skip: float32 [48], replicated, may hold values from 0 to 2
- norm_gain: float32 [3072], replicated, may hold values from 0.25 to 1.75
- w_out: bfloat16 [3072, 1536], P('fsdp'), may hold values from -0.109375 to 0.109375
- cotangent: bfloat16 [4, 2048, 1536], P('fsdp', 'seq'), may hold values from -6 to 6
Outputs:
- output: bfloat16 [4, 2048, 1536], P('fsdp', 'seq')
- input_grad: bfloat16 [4, 2048, 1536], P('fsdp', 'seq')
- grad_in_w: float32 [1536, 6448], P('fsdp')
- grad_out_w: float32 [3072, 1536], P('fsdp')
- grad_pre_gain: float32 [1536], replicated
- grad_conv_weight: float32 [4, 3328], replicated
- grad_conv_bias: float32 [3328], replicated
- grad_dt_bias: float32 [48], replicated
- grad_a_log: float32 [48], replicated
- grad_d_skip: float32 [48], replicated
- grad_norm_gain: float32 [3072], replicated
The draws below stay inside these ranges and needn't reach their ends.
Inputs may be any that keep to these rules, and one draw needn't show every extreme that they name: `seg_ids`: along each sequence the document numbers never fall; each document holds at most 1024 positions and one holds exactly that many.
All inputs are finite; a program needn't handle non-finite values.
Results may differ from the reference program's by a relative error of at most 0.012.
The reference program's roundings to bfloat16 on the way count: a program that leaves them out, or rounds other values in their place, can miss the bound.
Values may be sent and summed in bfloat16 or wider, within the bound.
A program may use at most 256 MiB of HBM per device.

```python
import math
import jax
import jax.numpy as jnp
import numpy as np
from jax import lax

D = 1536
H = 48
P_SIZE = 64
N = 128
CONVK = 4
SPAN = 256
LEN = 2048
SEQS = 4
DI = 3072
PROJ = 6448
N_SEQ = 8


def levels(key, dims, shards, smallest, largest):
    def one(dim, shards_of):
        steps = jax.random.uniform(jax.random.fold_in(jax.random.fold_in(key, 6), dim), (shards_of,), jnp.float32, smallest / len(shards), largest / len(shards))
        return jnp.repeat(jnp.exp(steps), dims[dim] // shards_of).reshape((-1,) + (1,) * (len(dims) - dim - 1))

    level = one(*shards[0])
    for cut in shards[1:]:
        level = level * one(*cut)
    return level


def profile(number_of, total, bound, lean):
    loads = [(1 << 20) // math.isqrt(rank ** lean) + 1 for rank in range(2, number_of + 1)]
    spare, holding = total - bound - (number_of - 1), [1] * (number_of - 1)
    while spare > 0:
        candidates = [i for i in range(number_of - 1) if holding[i] < bound]
        whole, budget = sum([loads[i] for i in candidates]), spare
        for i in candidates:
            more = min(bound - holding[i], max(1, budget * loads[i] // whole), spare)
            holding[i] = holding[i] + more
            spare = spare - more
    return np.array([bound] + holding)


def uneven_parts(own_key, amount, total, reach, skew):
    if amount == 2:
        one = jax.random.randint(own_key, (), max(1, total - reach), min(reach, total - 1) + 1)
        return jnp.stack([one, total - one])
    sizes = jnp.asarray(profile(amount, total, reach, skew), jnp.int32)
    pairs = (amount - 1) // 2
    source_of, taker = sizes[1:1 + 2 * pairs:2], sizes[2:2 + 2 * pairs:2]
    margin = jnp.minimum(source_of - 1, reach - taker)
    moved = jax.random.randint(jax.random.fold_in(own_key, 1), (pairs,), 0, 1 << 20) % (margin + 1)
    sizes = sizes.at[1:1 + 2 * pairs:2].set(source_of - moved).at[2:2 + 2 * pairs:2].set(taker + moved)
    return sizes[jax.random.permutation(jax.random.fold_in(own_key, 2), amount)]


def centred(stream_key, dims, deviation, limit, cuts=(), kind=jnp.bfloat16):
    factor_of = levels(stream_key, dims, cuts, -0.22, 0.18) if cuts else 1.0
    values = jax.random.normal(stream_key, dims, jnp.float32) * deviation * factor_of
    return jnp.minimum(jnp.maximum(values, -limit), limit).astype(kind)


def setup_inputs(seed: int = 0) -> dict:
    splits = jax.random.split(jax.random.key(seed), 13)
    tokens = centred(splits[0], (SEQS, LEN, D), 1.0, 6.0, ((0, 4), (1, 8)))
    seg_ids = jax.vmap(lambda own: jnp.searchsorted(jnp.cumsum(uneven_parts(own, 4, LEN, LEN // 2, 2)), jnp.arange(LEN), side="right"))(jax.random.split(splits[1], SEQS)).reshape((SEQS, LEN)).astype(jnp.int32)
    pre_gain = jnp.clip(1.0 + 0.15 * jax.random.normal(splits[2], (D,), jnp.float32), 0.25, 1.75)
    w_in = centred(splits[3], (D, PROJ), D ** -0.5, 0.15625, ((0, 4),))
    conv_weight = centred(splits[4], (CONVK, DI + 2 * N), 0.5, 3.0, (), jnp.float32)
    conv_bias = centred(splits[5], (DI + 2 * N,), 0.5, 3.0, (), jnp.float32)
    dt_bias = jnp.clip(jax.random.uniform(splits[6], (H,), jnp.float32, -6.0, -2.0), -6.0, -2.0)
    a_log = jnp.clip(jax.random.uniform(splits[7], (H,), jnp.float32, -5.0, 1.5), -5.0, 1.5)
    d_skip = jnp.clip(jax.random.uniform(splits[8], (H,), jnp.float32, 0.0, 2.0), 0.0, 2.0)
    norm_gain = jnp.clip(1.0 + 0.15 * jax.random.normal(splits[9], (DI,), jnp.float32), 0.25, 1.75)
    w_out = centred(splits[10], (DI, D), DI ** -0.5, 0.109375, ((0, 4),))
    cotangent = centred(splits[11], (SEQS, LEN, D), 1.0, 6.0, ((0, 4), (1, 8)))
    return {"tokens": tokens, "seg_ids": seg_ids, "pre_gain": pre_gain, "w_in": w_in, "conv_weight": conv_weight, "conv_bias": conv_bias, "dt_bias": dt_bias, "a_log": a_log, "d_skip": d_skip, "norm_gain": norm_gain, "w_out": w_out, "cotangent": cotangent}


EPSILON = 1e-05
HIGHEST = lax.Precision.HIGHEST

def causal_conv(values, kernel, offset_bias, segment):
    length = values.shape[0]
    taps = kernel.shape[0]
    padded = jnp.pad(values, ((taps - 1, 0), (0, 0)))
    seg_padded = jnp.pad(segment, (taps - 1, 0), constant_values=-1)
    total = jnp.zeros_like(values) + offset_bias[None, :]
    for lag_index in range(taps):
        same_doc = (seg_padded[lag_index:lag_index + length] == segment).astype(jnp.float32)
        total = total + kernel[lag_index][None, :] * padded[lag_index:lag_index + length] * same_doc[:, None]
    return jax.nn.silu(total)

def mixer(x_raw, bc_raw, dt_raw, kernel_x, bias_x, kernel_bc, bias_bc, step_bias, decay_log, skip_weight, segment):
    length = x_raw.shape[0]
    head_count = dt_raw.shape[1]
    x_conv = causal_conv(x_raw, kernel_x, bias_x, segment)
    bc_conv = causal_conv(bc_raw, kernel_bc, bias_bc, segment)
    key_rows = bc_conv[:, :N]
    query_rows = bc_conv[:, N:]
    step_size = jax.nn.softplus(dt_raw + step_bias[None, :])
    rate = -step_size * jnp.exp(decay_log)[None, :]
    blocks = length // SPAN
    x_blocks = x_conv.reshape(blocks, SPAN, head_count, P_SIZE)
    key_blocks = key_rows.reshape(blocks, SPAN, N)
    query_blocks = query_rows.reshape(blocks, SPAN, N)
    step_blocks = step_size.reshape(blocks, SPAN, head_count)
    rate_blocks = rate.reshape(blocks, SPAN, head_count)
    seg_blocks = segment.reshape(blocks, SPAN)
    cumulative = jnp.cumsum(rate_blocks, axis=1)
    scores = jnp.einsum('cqn,ckn->cqk', query_blocks, key_blocks, precision=HIGHEST)
    causal = jnp.arange(SPAN)[:, None] >= jnp.arange(SPAN)[None, :]
    live = causal[None] & (seg_blocks[:, :, None] == seg_blocks[:, None, :])
    gap = cumulative[:, :, None, :] - cumulative[:, None, :, :]
    decay = jnp.exp(jnp.where(live[..., None], gap, -1000000000.0))
    mixing = scores[..., None] * decay * step_blocks[:, None, :, :]
    inside = jnp.einsum('cqkh,ckhp->cqhp', mixing, x_blocks, precision=HIGHEST)
    last_seg = seg_blocks[:, -1]
    to_end = jnp.exp(cumulative[:, -1:, :] - cumulative) * (seg_blocks == last_seg[:, None]).astype(jnp.float32)[..., None]
    states = jnp.einsum('ckn,ckh,ckhp->chnp', key_blocks, to_end * step_blocks, x_blocks, precision=HIGHEST)
    through = jnp.exp(cumulative[:, -1, :])
    keeping = jnp.concatenate([jnp.zeros((1,), jnp.float32), (last_seg[1:] == last_seg[:-1]).astype(jnp.float32)])

    def carry_step(previous, pieces):
        state_now, passed, kept = pieces
        updated = state_now + previous * (passed * kept)[:, None, None]
        return (updated, previous)
    _, entering = lax.scan(carry_step, jnp.zeros((head_count, N, P_SIZE), jnp.float32), (states, through, keeping))
    prev_seg = jnp.concatenate([last_seg[:1] * 0 - 1, last_seg[:-1]])
    from_prev = jnp.exp(cumulative) * (seg_blocks == prev_seg[:, None]).astype(jnp.float32)[..., None]
    carried = jnp.einsum('cqn,chnp->cqhp', query_blocks, entering, precision=HIGHEST) * from_prev[..., None]
    result = inside + carried + skip_weight[None, None, :, None] * x_blocks
    return result.reshape(length, head_count * P_SIZE)

def reference(tokens, seg_ids, pre_gain, w_in, conv_weight, conv_bias, dt_bias, a_log, d_skip, norm_gain, w_out, cotangent):
    groups = N_SEQ
    head_local = H // groups
    chan_local = head_local * P_SIZE
    kernel_x = conv_weight[:, :DI]
    bias_x = conv_bias[:DI]
    kernel_bc = conv_weight[:, DI:]
    bias_bc = conv_bias[DI:]

    def one_sequence(totals, inputs):
        sequence, segment, cot_half = inputs
        tok_float = sequence.astype(jnp.float32)
        inv_rms = lax.rsqrt(lax.optimization_barrier(jnp.mean(tok_float * tok_float, -1, keepdims=True)) + EPSILON)
        scaled = tok_float * inv_rms
        normed = (scaled * pre_gain[None, :]).astype(jnp.bfloat16)
        projected = jnp.dot(normed, w_in, preferred_element_type=jnp.float32).astype(jnp.bfloat16)
        z_float = projected[:, :DI].astype(jnp.float32)
        x_raw = projected[:, DI:2 * DI].astype(jnp.float32)
        bc_raw = projected[:, 2 * DI:2 * DI + 2 * N].astype(jnp.float32)
        dt_raw = projected[:, 2 * DI + 2 * N:].astype(jnp.float32)

        def group_args(group):
            chan_start = (group * chan_local).astype(jnp.int32)
            head_start = (group * head_local).astype(jnp.int32)
            return (lax.dynamic_slice_in_dim(x_raw, chan_start, chan_local, 1), bc_raw, lax.dynamic_slice_in_dim(dt_raw, head_start, head_local, 1), lax.dynamic_slice_in_dim(kernel_x, chan_start, chan_local, 1), lax.dynamic_slice_in_dim(bias_x, chan_start, chan_local, 0), kernel_bc, bias_bc, lax.dynamic_slice_in_dim(dt_bias, head_start, head_local, 0), lax.dynamic_slice_in_dim(a_log, head_start, head_local, 0), lax.dynamic_slice_in_dim(d_skip, head_start, head_local, 0))

        def group_forward(group):
            return mixer(*group_args(group), segment)
        group_ids = jnp.arange(groups, dtype=jnp.int32)
        mixed = lax.map(group_forward, group_ids)
        mixed_half = jnp.transpose(mixed, (1, 0, 2)).reshape(-1, DI).astype(jnp.bfloat16)
        y_float = lax.optimization_barrier(mixed_half).astype(jnp.float32)
        sigma = jax.nn.sigmoid(z_float)
        gated_z = z_float * sigma
        gated = y_float * gated_z
        inv_gate = lax.rsqrt(lax.optimization_barrier(jnp.mean(gated * gated, -1, keepdims=True)) + EPSILON)
        unit_gate = gated * inv_gate
        normed_gate = (unit_gate * norm_gain[None, :]).astype(jnp.bfloat16)
        output = (tok_float + jnp.dot(normed_gate, w_out, preferred_element_type=jnp.float32)).astype(jnp.bfloat16)
        cot_float = cot_half.astype(jnp.float32)
        grad_out_w = jnp.dot(normed_gate.T, cot_half, preferred_element_type=jnp.float32)
        grad_gate_half = jnp.dot(cot_half, w_out.T, preferred_element_type=jnp.float32).astype(jnp.bfloat16)
        grad_gate = lax.optimization_barrier(grad_gate_half).astype(jnp.float32)
        grad_ngain = lax.optimization_barrier(jnp.sum(grad_gate * unit_gate, 0))
        scaled_grad = grad_gate * norm_gain[None, :]
        grad_gated = inv_gate * (scaled_grad - unit_gate * lax.optimization_barrier(jnp.mean(scaled_grad * unit_gate, -1, keepdims=True)))
        grad_y_half = (grad_gated * gated_z).astype(jnp.bfloat16)
        grad_y = lax.optimization_barrier(grad_y_half).astype(jnp.float32)
        grad_z_half = (grad_gated * y_float * sigma * (1.0 + z_float * (1.0 - sigma))).astype(jnp.bfloat16)

        def group_backward(carry, group):
            operands = group_args(group)
            _, pullback = jax.vjp(lambda *values: mixer(*values, segment), *operands)
            chan_start = (group * chan_local).astype(jnp.int32)
            grads = pullback(lax.dynamic_slice_in_dim(grad_y, chan_start, chan_local, 1))
            g_x, g_bc, g_dt, g_kx, g_bx, g_kbc, g_bbc, g_step, g_decay, g_skip = grads
            carry = (carry[0] + g_bc, carry[1] + g_kbc, carry[2] + g_bbc)
            return (carry, (g_x, g_dt, g_kx, g_bx, g_step, g_decay, g_skip))
        init_carry = (jnp.zeros((bc_raw.shape[0], 2 * N), jnp.float32), jnp.zeros((CONVK, 2 * N), jnp.float32), jnp.zeros((2 * N,), jnp.float32))
        (g_bc, g_kbc, g_bbc), stacked = lax.scan(group_backward, init_carry, group_ids)
        g_x, g_dt, g_kx, g_bx, g_step, g_decay, g_skip = stacked
        x_grad = jnp.transpose(g_x, (1, 0, 2)).reshape(-1, DI).astype(jnp.bfloat16)
        dt_grad = jnp.transpose(g_dt, (1, 0, 2)).reshape(-1, H).astype(jnp.bfloat16)
        proj_grad = jnp.concatenate([grad_z_half, x_grad, g_bc.astype(jnp.bfloat16), dt_grad], -1)
        grad_in_w = jnp.dot(normed.T, proj_grad, preferred_element_type=jnp.float32)
        grad_normed = jnp.dot(proj_grad, w_in.T, preferred_element_type=jnp.float32)
        grad_pre = lax.optimization_barrier(jnp.sum(grad_normed * scaled, 0))
        weighted = grad_normed * pre_gain[None, :]
        input_grad = (cot_float + inv_rms * (weighted - scaled * lax.optimization_barrier(jnp.mean(weighted * scaled, -1, keepdims=True)))).astype(jnp.bfloat16)
        conv_w_grad = jnp.concatenate([jnp.transpose(g_kx, (1, 0, 2)).reshape(CONVK, DI), g_kbc], 1)
        conv_b_grad = jnp.concatenate([g_bx.reshape(DI), g_bbc], 0)
        updates = (grad_in_w, grad_out_w, grad_pre, conv_w_grad, conv_b_grad, g_step.reshape(H), g_decay.reshape(H), g_skip.reshape(H), grad_ngain)
        totals = tuple((old + new for old, new in zip(totals, updates)))
        return (totals, (output, input_grad))
    init_totals = (jnp.zeros((D, PROJ), jnp.float32), jnp.zeros((DI, D), jnp.float32), jnp.zeros((D,), jnp.float32), jnp.zeros((CONVK, DI + 2 * N), jnp.float32), jnp.zeros((DI + 2 * N,), jnp.float32), jnp.zeros((H,), jnp.float32), jnp.zeros((H,), jnp.float32), jnp.zeros((H,), jnp.float32), jnp.zeros((DI,), jnp.float32))
    totals, (outputs, input_grads) = lax.scan(one_sequence, init_totals, (tokens, seg_ids, cotangent))
    grad_in_w, grad_out_w, grad_pre, conv_w_grad, conv_b_grad, grad_step, grad_decay, grad_skip, grad_ngain = totals
    return (outputs, input_grads, grad_in_w, grad_out_w, grad_pre, conv_w_grad, conv_b_grad, grad_step, grad_decay, grad_skip, grad_ngain)
```

```python
import functools

import jax
import jax.numpy as jnp
from jax import lax
from jax.experimental import pallas as pl
from jax.experimental.pallas import tpu as pltpu
from jax.sharding import PartitionSpec as P

P_SIZE = 64
N = 128
TAPS = 4
HALO = TAPS - 1
EDGE = 8
LANES = 128
EPSILON = 1e-05
F32 = jnp.float32
BF16 = jnp.bfloat16
MESH = pl.DeviceIdType.MESH
ANY = pl.BlockSpec(memory_space=pl.ANY)
VMEM = pl.BlockSpec(memory_space=pltpu.VMEM)
VMEM_BYTES = 56 << 20


def half(value):
    return value.astype(BF16)


def mm(left, right, dims):
    return lax.dot_general(half(left), half(right), (dims, ((), ())), preferred_element_type=F32)


NN = ((1,), (0,))
NT = ((1,), (1,))
TN = ((0,), (0,))


def split_dot(value, table, dims):
    top = half(value)
    rest = half(value - top.astype(F32))
    return mm(top, table, dims) + mm(rest, table, dims)


def head_table(channels):
    row = lax.broadcasted_iota(jnp.int32, (LANES, channels), 0)
    col = lax.broadcasted_iota(jnp.int32, (LANES, channels), 1)
    low = row * P_SIZE
    return half(((col >= low) & (col < low + P_SIZE)).astype(F32))


def triangle(length, lower):
    row = lax.broadcasted_iota(jnp.int32, (length, length), 0)
    col = lax.broadcasted_iota(jnp.int32, (length, length), 1)
    return half(((row >= col) if lower else (row <= col)).astype(F32))


def running_sum(values, lower):
    table = triangle(values.shape[0], lower)
    a = half(values)
    rest = values - a.astype(F32)
    b = half(rest)
    c = half(rest - b.astype(F32))
    return mm(table, a, NN) + mm(table, b, NN) + mm(table, c, NN)


def softplus(value):
    return jnp.maximum(value, 0.0) + jnp.log1p(jnp.exp(-jnp.abs(value)))


def params(**more):
    return pltpu.CompilerParams(vmem_limit_bytes=VMEM_BYTES, **more)


def meet(targets):
    barrier = pltpu.get_barrier_semaphore()
    for target in targets:
        pl.semaphore_signal(barrier, inc=1, device_id=target, device_id_type=MESH)
    pl.semaphore_wait(barrier, len(targets))


def remote(src, dst, send, recv, target):
    return pltpu.make_async_remote_copy(
        src_ref=src, dst_ref=dst, send_sem=send, recv_sem=recv, device_id=target, device_id_type=MESH
    )


def gather_kernel(n_s, n_f, C, DI, tok, seg, w, tok_all, seg_all, w_z, w_x, w_b, edge, edge_own, b_tok, b_z, b_x, b_b, b_seg, snd, rcv, loc):
    s, f = lax.axis_index("seq"), lax.axis_index("fsdp")
    L, R = tok.shape[0], w.shape[0]
    tail = w.shape[1] - 2 * DI
    right, left = lax.rem(s + 1, n_s), lax.rem(s + n_s - 1, n_s)
    parity = lax.rem(s, 2)
    pair = s + 1 - 2 * parity
    peers = [lax.rem(f + k, n_f) for k in range(1, n_f)]
    meet([(right, f), (left, f)] + [(s, p) for p in peers])
    count = [0]

    def go(src, dst, target):
        i = count[0]
        count[0] = i + 1
        copy = remote(src, dst, snd.at[i], rcv.at[i], target)
        copy.start()
        return copy

    halves = pl.ds(pl.multiple_of(parity * (R // 2), R // 2), R // 2)
    others = pl.ds(pl.multiple_of((1 - parity) * (R // 2), R // 2), R // 2)
    cols = [pl.ds(pl.multiple_of(p * C, C), C) for p in range(2 * n_f)]

    def part(j, base):
        return pl.ds(pl.multiple_of(base + j * C, C), C)

    first = go(tok.at[pl.ds(L - EDGE, EDGE)], edge_own, (right, f))
    started = []
    for p in peers:
        started.append(go(seg, seg_all.at[f], (s, p)))
        started.append(go(tok, tok_all.at[f], (s, p)))
    w_copies = []
    for p in peers:
        w_copies.append(
            [
                go(w.at[halves, part(p, 0)], w_z.at[f, halves], (s, p)),
                go(w.at[halves, part(p, DI)], w_x.at[f, halves], (s, p)),
                go(w.at[halves, pl.ds(2 * DI, tail)], w_b.at[f, halves], (s, p)),
            ]
        )
    mine = [
        (tok, b_tok, tok_all.at[f]),
        (seg, b_seg, seg_all.at[f]),
        (w.at[:, part(f, 0)], b_z, w_z.at[f]),
        (w.at[:, part(f, DI)], b_x, w_x.at[f]),
        (w.at[:, pl.ds(2 * DI, tail)], b_b, w_b.at[f]),
    ]
    ins = [pltpu.make_async_copy(a, b, loc.at[i]) for i, (a, b, _) in enumerate(mine)]
    for c in ins:
        c.start()
    first.wait()
    edges = [go(edge_own, edge.at[f], (s, p)) for p in peers]
    own_edge = pltpu.make_async_copy(edge_own, edge.at[f], loc.at[len(mine)])
    own_edge.start()
    outs = []
    for i, (_, b, c) in enumerate(mine):
        ins[i].wait()
        out = pltpu.make_async_copy(b, c, loc.at[len(mine) + 1 + i])
        out.start()
        outs.append(out)
    relays = []
    for k, copies in enumerate(w_copies):
        source = lax.rem(f + n_f - (k + 1), n_f)
        for copy, array in zip(copies, (w_z, w_x, w_b)):
            copy.wait_recv()
            relays.append(go(array.at[source, halves], array.at[source, halves], (pair, f)))
    for copy in relays:
        copy.wait()
    for copies in w_copies:
        for copy in copies:
            copy.wait_send()
    for copy in started + edges:
        copy.wait()
    own_edge.wait()
    for out in outs:
        out.wait()


def gather(tok, seg, w, C, DI, n_s, n_f):
    L, D = tok.shape
    R = w.shape[0]
    tail = w.shape[1] - 2 * DI
    copies = 1 + 6 * (n_f - 1) + 3 * (n_f - 1)
    sems = copies
    outs = [
        jax.ShapeDtypeStruct((n_f, L, D), BF16),
        jax.ShapeDtypeStruct((n_f,) + seg.shape, seg.dtype),
        jax.ShapeDtypeStruct((n_f, R, C), BF16),
        jax.ShapeDtypeStruct((n_f, R, C), BF16),
        jax.ShapeDtypeStruct((n_f, R, tail), BF16),
        jax.ShapeDtypeStruct((n_f, EDGE, D), BF16),
        jax.ShapeDtypeStruct((EDGE, D), BF16),
    ]
    return pl.pallas_call(
        functools.partial(gather_kernel, n_s, n_f, C, DI),
        name="gather",
        out_shape=outs,
        in_specs=[ANY] * 3,
        out_specs=[ANY] * 7,
        scratch_shapes=[
            pltpu.VMEM((L, D), BF16),
            pltpu.VMEM((R, C), BF16),
            pltpu.VMEM((R, C), BF16),
            pltpu.VMEM((R, tail), BF16),
            pltpu.VMEM(seg.shape, seg.dtype),
            pltpu.SemaphoreType.DMA((sems,)),
            pltpu.SemaphoreType.DMA((sems,)),
            pltpu.SemaphoreType.DMA((11,)),
        ],
        compiler_params=params(collective_id=0, has_side_effects=True),
    )(tok, seg, w)


def chain_kernel(n_s, forward, state, through, result, out, snd, rcv):
    s, f = lax.axis_index("seq"), lax.axis_index("fsdp")
    right, left = lax.rem(s + 1, n_s), lax.rem(s + n_s - 1, n_s)
    meet([(right, f), (left, f)])
    target = right if forward else left
    first = s == (0 if forward else n_s - 1)
    last = s == (n_s - 1 if forward else 0)
    copies = []
    for q in range(state.shape[0]):
        copy = remote(out.at[q], result.at[q], snd.at[q], rcv.at[q], (target, f))
        copies.append(copy)

        @pl.when(first)
        def _():
            result[q] = jnp.zeros_like(result[q])

        @pl.when(jnp.logical_not(first))
        def _():
            copy.wait_recv()

        out[q] = half(state[q] + result[q].astype(F32) * through[q, 0:1, :])

        @pl.when(jnp.logical_not(last))
        def _():
            copy.start()

    @pl.when(jnp.logical_not(last))
    def _():
        for copy in copies:
            copy.wait_send()


def chain(states, through, forward, n_s):
    return pl.pallas_call(
        functools.partial(chain_kernel, n_s, forward),
        name="chain_on" if forward else "chain_back",
        out_shape=jax.ShapeDtypeStruct(states.shape, BF16),
        in_specs=[VMEM] * 2,
        out_specs=VMEM,
        scratch_shapes=[
            pltpu.VMEM(states.shape, BF16),
            pltpu.SemaphoreType.DMA((states.shape[0],)),
            pltpu.SemaphoreType.DMA((states.shape[0],)),
        ],
        compiler_params=params(collective_id=1 if forward else 2, has_side_effects=True),
    )(states, through)


def total_kernel(n_f, part, total, got, snd, rcv):
    s, f = lax.axis_index("seq"), lax.axis_index("fsdp")
    peers = [lax.rem(f + k, n_f) for k in range(1, n_f)]
    meet([(s, p) for p in peers])
    copies = []
    for k, p in enumerate(peers):
        copy = remote(part, got.at[k], snd.at[k], rcv.at[k], (s, p))
        copy.start()
        copies.append(copy)
    value = part[...]
    for k, copy in enumerate(copies):
        copy.wait()
        value = value + got[k]
    total[...] = value


def total_over_fsdp(part, n_f):
    return pl.pallas_call(
        functools.partial(total_kernel, n_f),
        name="total",
        out_shape=jax.ShapeDtypeStruct(part.shape, F32),
        in_specs=[VMEM],
        out_specs=VMEM,
        scratch_shapes=[
            pltpu.VMEM((n_f - 1,) + part.shape, F32),
            pltpu.SemaphoreType.DMA((n_f - 1,)),
            pltpu.SemaphoreType.DMA((n_f - 1,)),
        ],
        compiler_params=params(collective_id=3, has_side_effects=True),
    )(part)


def fill(scratch, halo, raw):
    length = raw.shape[0]
    scratch[0:EDGE, :] = halo.astype(F32)
    scratch[EDGE : EDGE + length, :] = raw.astype(F32)


def conv(scratch, length, kernel, cols):
    pre = kernel[TAPS : TAPS + 1, :] + kernel[HALO : HALO + 1, :] * scratch[EDGE : EDGE + length, :]
    for k in range(HALO):
        start = EDGE - HALO + k
        pre = pre + kernel[k : k + 1, :] * (scratch[start : start + length, :] * cols[:, k : k + 1])
    return pre


def silu(value):
    return value * jax.nn.sigmoid(value)


def enter_kernel(x, x_halo, b, b_halo, d, cols, k_x, k_b, heads, state, through, pre_x, xd, pre_b, bc, cum, cum_row, s_x, s_b):
    L, C = x.shape
    table = head_table(C)
    c = cols[...]
    fill(s_x, x_halo[...], x[...])
    fill(s_b, b_halo[...], b[...])
    px = conv(s_x, L, k_x, c)
    pb = conv(s_b, L, k_b, c)
    pre_x[...] = px
    pre_b[...] = pb
    bc[...] = half(silu(pb))
    step = softplus(d[...].astype(F32) + heads[0:1, :])
    rate = -step * heads[1:2, :]
    total = running_sum(rate, True)
    cum[...] = total
    cum_row[...] = jnp.transpose(total)[0 : cum_row.shape[0], :]
    last = total[L - 1 : L, :]
    to_end = jnp.exp(last - total) * c[:, 3:4]
    entry_last = jnp.exp(last) * c[L - 1 : L, 4:5]
    through[...] = split_dot(jnp.broadcast_to(entry_last, (8, LANES)), table, NN)
    xdv = split_dot(step, table, NN) * silu(px)
    xd[...] = half(xdv)
    wx = half(split_dot(to_end, table, NN) * xdv)
    state[...] = mm(bc[:, 0:N], wx, TN)


def block_rows(L):
    return min(L, 128)


def live_rows(cols, seg_row, r, rows, width):
    row = lax.broadcasted_iota(jnp.int32, (rows, width), 0) + r * rows
    col = lax.broadcasted_iota(jnp.int32, (rows, width), 1)
    same = cols[r * rows : (r + 1) * rows, 5:6] == seg_row[0:1, 0:width]
    return (row >= col) & same


def mix_kernel(pre_x, xd, bc, cum, cum_row, cols, seg_row, enter, z, gg, gain, heads, plain, mixed, sums):
    L, C = xd.shape
    rows = block_rows(L)
    table = head_table(C)
    cv = cum[...]
    entry = jnp.exp(cv) * cols[:, 4:5]
    carried = mm(bc[:, N : 2 * N], enter[...], NN) * split_dot(entry, table, NN)
    for r in range(L // rows):
        width = (r + 1) * rows
        mine = slice(r * rows, (r + 1) * rows)
        scores = jnp.where(
            live_rows(cols, seg_row, r, rows, width), mm(bc[mine, N : 2 * N], bc[0:width, 0:N], NT), 0.0
        )
        for h in range(0, C // P_SIZE, 2):
            pieces = []
            for g in (h, h + 1):
                gap = jnp.minimum(cum[mine, g : g + 1] - cum_row[g : g + 1, 0:width], 0.0)
                pieces.append(mm(scores * jnp.exp(gap), xd[0:width, g * P_SIZE : (g + 1) * P_SIZE], NN))
            plain[mine, h * P_SIZE : (h + 2) * P_SIZE] = jnp.concatenate(pieces, 1)
    y = plain[...] + carried
    plain[...] = y
    skip = split_dot(jnp.broadcast_to(heads[2:3, :], (8, LANES)), table, NN)[0:1, :]
    m = half(y + skip * silu(pre_x[...]))
    mixed[...] = m
    gated = m.astype(F32) * silu(z[...].astype(F32))
    sg = gg[...].astype(F32) * gain[0:1, :]
    one = jnp.sum(gated * gated, 1, keepdims=True)
    two = jnp.sum(sg * gated, 1, keepdims=True)
    lane = lax.broadcasted_iota(jnp.int32, (L, LANES), 1)
    both = jnp.where(lane == 0, one, jnp.where(lane == 1, two, 0.0))
    sums[...] = jnp.transpose(both)[0:8, :]


def gate_kernel(DI, mixed, z, gg, gain, total, cum, cols, bc, ngate, dz, dy, d_enter, d_gain):
    L, C = mixed.shape
    table = head_table(C)
    sums = jnp.transpose(jnp.concatenate([total[...], jnp.zeros((LANES - 8, L), F32)], 0))
    inv = lax.rsqrt(sums[:, 0:1] / DI + EPSILON)
    inner = inv * (sums[:, 1:2] / DI)
    y = mixed[...].astype(F32)
    zf = z[...].astype(F32)
    sig = jax.nn.sigmoid(zf)
    gz = zf * sig
    unit = y * gz * inv
    g = gg[...].astype(F32)
    ngate[...] = half(unit * gain[0:1, :])

    @pl.when(pl.program_id(0) == 0)
    def _():
        d_gain[...] = jnp.zeros_like(d_gain)

    d_gain[...] += jnp.broadcast_to(jnp.sum(g * unit, 0, keepdims=True), d_gain.shape)
    grad = inv * (g * gain[0:1, :] - unit * inner)
    d = half(grad * gz)
    dy[...] = d
    dz[...] = half(grad * y * sig * (1.0 + zf * (1.0 - sig)))
    entry = jnp.exp(cum[...]) * cols[:, 4:5]
    edy = half(split_dot(entry, table, NN) * d.astype(F32))
    d_enter[...] = mm(bc[:, N : 2 * N], edy, TN)


def silu_grad(pre, sigma):
    return sigma * (1.0 + pre * (1.0 - sigma))


def conv_back(dpre, raw, halo, kernel, cols, s_raw, s_grad, grads):
    length = dpre.shape[0]
    fill(s_raw, halo, raw)
    grads[TAPS : TAPS + 1, :] += jnp.sum(dpre, 0, keepdims=True)
    grads[HALO : HALO + 1, :] += jnp.sum(dpre * s_raw[EDGE : EDGE + length, :], 0, keepdims=True)
    d_raw = kernel[HALO : HALO + 1, :] * dpre
    width = dpre.shape[1]
    d_halo = jnp.zeros((EDGE, width), F32)
    s_grad[0:EDGE, :] = jnp.zeros((EDGE, width), F32)
    s_grad[EDGE + length : EDGE + length + EDGE, :] = jnp.zeros((EDGE, width), F32)
    for k in range(HALO):
        masked = dpre * cols[:, k : k + 1]
        start = EDGE - HALO + k
        grads[k : k + 1, :] += jnp.sum(masked * s_raw[start : start + length, :], 0, keepdims=True)
        s_grad[EDGE : EDGE + length, :] = masked
        up = HALO - k
        d_raw = d_raw + kernel[k : k + 1, :] * s_grad[EDGE + up : EDGE + up + length, :]
        d_halo = d_halo + kernel[k : k + 1, :] * s_grad[up : up + EDGE, :]
    return d_raw, d_halo


def back_kernel(
    x, x_halo, b, b_halo, d, cols, seg_row, k_x, k_b, heads, pre_x, xd, pre_b, bc, cum, cum_row, enter, grad, plain, dy,
    dx, db, dd, tail, halo, g_x, g_b, g_h, s_x, s_gx, s_b, s_gb, s_dxd, s_ds,
):
    L, C = xd.shape
    rows = block_rows(L)
    table = head_table(C)
    c = cols[...]
    cv = cum[...]

    @pl.when(pl.program_id(0) == 0)
    def _():
        g_x[...] = jnp.zeros_like(g_x)
        g_b[...] = jnp.zeros_like(g_b)
        g_h[...] = jnp.zeros_like(g_h)

    s_dxd[...] = jnp.zeros_like(s_dxd)
    s_ds[...] = jnp.zeros_like(s_ds)
    for r in range(L // rows):
        width = (r + 1) * rows
        mine = slice(r * rows, (r + 1) * rows)
        live = live_rows(cols, seg_row, r, rows, width)
        scores = jnp.where(live, mm(bc[mine, N : 2 * N], bc[0:width, 0:N], NT), 0.0)
        d_scores = jnp.zeros((rows, width), F32)
        for h in range(0, C // P_SIZE, 2):
            pieces = []
            for g in (h, h + 1):
                lanes = slice(g * P_SIZE, (g + 1) * P_SIZE)
                decay = jnp.exp(jnp.minimum(cum[mine, g : g + 1] - cum_row[g : g + 1, 0:width], 0.0))
                pieces.append(mm(scores * decay, dy[mine, lanes], TN))
                d_scores = d_scores + mm(dy[mine, lanes], xd[0:width, lanes], NT) * decay
            s_dxd[0:width, h * P_SIZE : (h + 2) * P_SIZE] += jnp.concatenate(pieces, 1)
        s_ds[mine, 0:width] = jnp.where(live, d_scores, 0.0)
    ds = half(s_ds[...])
    last = cv[L - 1 : L, :]
    to_end = split_dot(jnp.exp(last - cv) * c[:, 3:4], table, NN)
    entry = split_dot(jnp.exp(cv) * c[:, 4:5], table, NN)
    dyf = dy[...].astype(F32)
    xdf = xd[...].astype(F32)
    dwx = mm(bc[:, 0:N], grad[...], NN)
    wx = half(to_end * xdf)
    d_b = mm(wx, grad[...], NT) + mm(ds, bc[:, N : 2 * N], TN)
    d_c = mm(half(entry * dyf), enter[...], NT) + mm(ds, bc[:, 0:N], NN)
    u = split_dot(wx.astype(F32) * dwx, table, NT)
    dxd_in = s_dxd[...]
    dcum = split_dot(dyf * plain[...] - xdf * dxd_in, table, NT) - u
    carry = jnp.sum(enter[...].astype(F32) * grad[...].astype(F32), 0, keepdims=True)
    carry = split_dot(jnp.broadcast_to(carry, (8, C)), table, NT)[0:1, :]
    at_last = jnp.sum(u, 0, keepdims=True) + jnp.exp(last) * c[L - 1 : L, 4:5] * carry
    row = lax.broadcasted_iota(jnp.int32, (L, LANES), 0)
    dcum = dcum + jnp.where(row == L - 1, at_last, 0.0)
    drate = running_sum(dcum, False)
    px = pre_x[...]
    sig = jax.nn.sigmoid(px)
    xf = px * sig
    dxd = dxd_in + to_end * dwx
    raw_step = d[...].astype(F32) + heads[0:1, :]
    step = softplus(raw_step)
    ddt = split_dot(xf * dxd, table, NT) - drate * heads[1:2, :]
    ddt_raw = ddt * jax.nn.sigmoid(raw_step)
    dd[...] = half(ddt_raw)
    g_h[0:1, :] += jnp.sum(ddt_raw, 0, keepdims=True)
    g_h[1:2, :] += jnp.sum(drate * (-step * heads[1:2, :]), 0, keepdims=True)
    g_h[2:3, :] += split_dot(jnp.broadcast_to(jnp.sum(dyf * xf, 0, keepdims=True), (8, C)), table, NT)[0:1, :]
    skip = split_dot(jnp.broadcast_to(heads[2:3, :], (8, LANES)), table, NN)[0:1, :]
    d_x = split_dot(step, table, NN) * dxd + skip * dyf
    rx, hx = conv_back(d_x * silu_grad(px, sig), x[...], x_halo[...], k_x, c, s_x, s_gx, g_x)
    pb = pre_b[...]
    d_bc = jnp.concatenate([d_b, d_c], 1) * silu_grad(pb, jax.nn.sigmoid(pb))
    rb, hb = conv_back(d_bc, b[...], b_halo[...], k_b, c, s_b, s_gb, g_b)
    dx[...] = half(rx)
    db[...] = half(rb)
    tail[:, 0:C] = rx[L - EDGE : L, :]
    tail[:, C : C + 2 * N] = rb[L - EDGE : L, :]
    halo[:, 0:C] = half(hx)
    halo[:, C : C + 2 * N] = half(hb)


def per(*shape, col=0):
    return pl.BlockSpec((None,) + shape, lambda q: (q, 0, col))


def fixed(*shape):
    return pl.BlockSpec(shape, lambda q: (0,) * len(shape))


def shaped(*shape, dtype=F32):
    return jax.ShapeDtypeStruct(shape, dtype)


def shards(tokens, seg_ids, pre_gain, w_in, conv_weight, conv_bias, dt_bias, a_log, d_skip, norm_gain, w_out, cotangent):
    n_s = lax.axis_size("seq")
    n_f = lax.axis_size("fsdp")
    s = lax.axis_index("seq")
    f = lax.axis_index("fsdp")
    L, D = tokens.shape[1:]
    DI = norm_gain.shape[0]
    H = dt_bias.shape[0]
    Hl = H // n_f
    C = DI // n_f
    pair = conv_bias.shape[0] - DI
    T = n_f * L
    rows = w_in.shape[0]
    HR = -(-Hl // 8) * 8

    def mine(array, width, axis):
        return lax.dynamic_slice_in_dim(array, f * width, width, axis)

    tok_all, seg_full, w_z, w_x, w_b, edge, _ = gather(tokens[0], seg_ids, w_in, C, DI, n_s, n_f)
    w_z, w_x, w_b = w_z.reshape(D, C), w_x.reshape(D, C), w_b.reshape(D, pair + H)
    cot_own, _ = lax.optimization_barrier((cotangent[0], tok_all))
    cot_all = lax.all_gather(cot_own, "fsdp").reshape(T, D)
    seg_full = seg_full[:, 0]
    seg_pad = jnp.pad(seg_full, ((0, 0), (HALO, 0)), constant_values=-1)
    seg_ext = lax.dynamic_slice_in_dim(seg_pad, s * L, L + HALO, 1)
    seg = seg_ext[:, HALO:]
    marks = [seg_ext[:, k : k + L] == seg for k in range(HALO)]
    marks += [seg == seg[:, L - 1 :], seg == seg_ext[:, HALO - 1 : HALO], seg]
    cols = jnp.stack([m.astype(F32) for m in marks] + [jnp.zeros_like(seg, F32)] * (LANES - len(marks)), -1)
    seg_row = jnp.broadcast_to(seg.astype(F32)[:, None, :], (n_f, 8, L))

    def norm(values):
        values = values.astype(F32)
        inv = lax.rsqrt(jnp.mean(values * values, -1, keepdims=True) + EPSILON)
        return half(values * inv * pre_gain)

    normed = norm(tok_all).reshape(T, D)
    normed_edge = norm(edge).reshape(n_f * EDGE, D)

    def dot(a, b):
        return jnp.dot(a, b, preferred_element_type=F32)

    def dot_t(a, b):
        return lax.dot_general(a, b, (((1,), (1,)), ((), ())), preferred_element_type=F32)

    def t_dot(a, b):
        return lax.dot_general(a, b, (((0,), (0,)), ((), ())), preferred_element_type=F32)

    def lanes_of(values):
        return jnp.pad(mine(values, Hl, values.ndim - 1), ((0, 0),) * (values.ndim - 1) + ((0, LANES - Hl),))

    z = half(dot(normed, w_z)).reshape(n_f, L, C)
    x_raw = half(dot(normed, w_x)).reshape(n_f, L, C)
    bd = half(dot(normed, w_b))
    bc_raw = bd[:, :pair].reshape(n_f, L, pair)
    dt_raw = lanes_of(bd[:, pair:]).reshape(n_f, L, LANES)
    x_halo = half(dot(normed_edge, w_x)).reshape(n_f, EDGE, C)
    bc_halo = half(dot(normed_edge, w_b[:, :pair])).reshape(n_f, EDGE, pair)
    ggate = half(dot_t(cot_all, w_out)).reshape(n_f, L, C)

    def kernel_rows(kernel, bias):
        return jnp.concatenate([kernel, bias[None], jnp.zeros((8 - TAPS - 1, bias.shape[0]), F32)], 0)

    k_x = kernel_rows(mine(conv_weight[:, :DI], C, 1), mine(conv_bias[:DI], C, 0))
    k_b = kernel_rows(conv_weight[:, DI:], conv_bias[DI:])
    bias_lane = jnp.where(jnp.arange(LANES) < Hl, lanes_of(dt_bias), -100.0)
    heads = jnp.stack([bias_lane, jnp.exp(lanes_of(a_log)), lanes_of(d_skip)] + [jnp.zeros((LANES,), F32)] * 5)
    gain = jnp.broadcast_to(mine(norm_gain, C, 0)[None], (8, C))

    big, small = per(L, C), per(L, pair)
    lane, col_spec, row_spec, st = per(L, LANES), per(L, LANES), per(8, L), per(N, C)
    halo_x, halo_b = per(EDGE, C), per(EDGE, pair)
    kx_spec, kb_spec, h_spec, hr_spec = fixed(8, C), fixed(8, pair), fixed(8, LANES), per(HR, L)
    call = functools.partial(pl.pallas_call, grid=(n_f,), compiler_params=params(dimension_semantics=("arbitrary",)))

    state, through, pre_x, xd, pre_b, bc, cum, cum_row = call(
        enter_kernel,
        name="enter",
        in_specs=[big, halo_x, small, halo_b, lane, col_spec, kx_spec, kb_spec, h_spec],
        out_specs=[st, per(8, C), big, big, small, small, lane, hr_spec],
        out_shape=[
            shaped(n_f, N, C), shaped(n_f, 8, C), shaped(n_f, L, C), shaped(n_f, L, C, dtype=BF16),
            shaped(n_f, L, pair), shaped(n_f, L, pair, dtype=BF16), shaped(n_f, L, LANES), shaped(n_f, HR, L),
        ],
        scratch_shapes=[pltpu.VMEM((L + EDGE, C), F32), pltpu.VMEM((L + EDGE, pair), F32)],
    )(x_raw, x_halo, bc_raw, bc_halo, dt_raw, cols, k_x, k_b, heads)
    enter = chain(state, through, True, n_s)
    plain, mixed, sums = call(
        mix_kernel,
        name="mix",
        in_specs=[big, big, small, lane, hr_spec, col_spec, row_spec, st, big, big, kx_spec, h_spec],
        out_specs=[big, big, row_spec],
        out_shape=[shaped(n_f, L, C), shaped(n_f, L, C, dtype=BF16), shaped(n_f, 8, L)],
    )(pre_x, xd, bc, cum, cum_row, cols, seg_row, enter, z, ggate, gain, heads)
    total = total_over_fsdp(sums, n_f)
    ngate, dz, dy, d_enter, g_gain = call(
        functools.partial(gate_kernel, DI),
        name="gate",
        in_specs=[big, big, big, kx_spec, row_spec, lane, col_spec, small],
        out_specs=[big, big, big, st, kx_spec],
        out_shape=[shaped(n_f, L, C, dtype=BF16)] * 3 + [shaped(n_f, N, C), shaped(8, C)],
    )(mixed, z, ggate, gain, total, cum, cols, bc)
    grad = chain(d_enter, through, False, n_s)
    ngate, dz = ngate.reshape(T, C), dz.reshape(T, C)

    out_part = half(dot(ngate, w_out)).reshape(n_f, L, D)
    out_sum = lax.psum_scatter(out_part, "fsdp", scatter_dimension=0, tiled=True)[0]
    tok_float = tokens[0].astype(F32)
    output = half(tok_float + out_sum.astype(F32))
    g_out = lax.psum(half(t_dot(ngate, cot_all)), "seq").astype(F32)

    dx, db, dd, tail, halo, g_x, g_b, g_h = call(
        back_kernel,
        name="back",
        in_specs=[
            big, halo_x, small, halo_b, lane, col_spec, row_spec, kx_spec, kb_spec, h_spec,
            big, big, small, small, lane, hr_spec, st, st, big, big,
        ],
        out_specs=[big, small, lane, per(EDGE, C + pair), per(EDGE, C + pair), kx_spec, kb_spec, h_spec],
        out_shape=[
            shaped(n_f, L, C, dtype=BF16), shaped(n_f, L, pair, dtype=BF16), shaped(n_f, L, LANES, dtype=BF16),
            shaped(n_f, EDGE, C + pair), shaped(n_f, EDGE, C + pair, dtype=BF16), shaped(8, C), shaped(8, pair), shaped(8, LANES),
        ],
        scratch_shapes=[
            pltpu.VMEM((L + EDGE, C), F32), pltpu.VMEM((L + 2 * EDGE, C), F32),
            pltpu.VMEM((L + EDGE, pair), F32), pltpu.VMEM((L + 2 * EDGE, pair), F32),
            pltpu.VMEM((L, C), F32), pltpu.VMEM((L, L), F32),
        ],
    )(x_raw, x_halo, bc_raw, bc_halo, dt_raw, cols, seg_row, k_x, k_b, heads,
      pre_x, xd, pre_b, bc, cum, cum_row, enter, grad, plain, dy)
    got = lax.ppermute(halo, "seq", [(i + 1, i) for i in range(n_s - 1)])
    fixed_tail = half(tail + got.astype(F32))
    dx = lax.dynamic_update_slice(dx, fixed_tail[..., :C], (0, L - EDGE, 0)).reshape(T, C)
    db = lax.dynamic_update_slice(db, fixed_tail[..., C:], (0, L - EDGE, 0)).reshape(T, pair)
    dd48 = lax.dynamic_update_slice(jnp.zeros((T, H), BF16), dd.reshape(T, LANES)[:, :Hl], (0, f * Hl))
    dbd = jnp.concatenate([db, dd48], 1)

    gn_part = dot_t(dz, w_z) + dot_t(dx, w_x) + dot_t(dbd, w_b)
    gn = lax.psum_scatter(half(gn_part).reshape(n_f, L, D), "fsdp", scatter_dimension=0, tiled=True)[0].astype(F32)
    inv_rms = lax.rsqrt(jnp.mean(tok_float * tok_float, -1, keepdims=True) + EPSILON)
    scaled = tok_float * inv_rms
    grad_pre = jnp.sum(gn * scaled, 0)
    weighted = gn * pre_gain[None, :]
    input_grad = half(
        cotangent[0].astype(F32)
        + inv_rms * (weighted - scaled * jnp.mean(weighted * scaled, -1, keepdims=True))
    )

    packed = [half(t_dot(normed, v)).reshape(n_f, rows, v.shape[1]) for v in (dz, dx, dbd)]
    gz, gx, gb = [lax.all_to_all(v, "fsdp", 0, 0, tiled=True) for v in packed]
    g_in = jnp.concatenate(
        [
            gz.transpose(1, 0, 2).reshape(rows, DI),
            gx.transpose(1, 0, 2).reshape(rows, DI),
            half(jnp.sum(gb.astype(F32), 0)),
        ],
        1,
    )
    g_in = lax.psum(g_in, "seq").astype(F32)

    def place(values, full, width):
        zeros = jnp.zeros(values.shape[:-1] + (full,), F32)
        return lax.dynamic_update_slice_in_dim(zeros, values, f * width, zeros.ndim - 1)

    conv_w = jnp.concatenate([place(g_x[:TAPS], DI, C), g_b[:TAPS]], 1)
    conv_b = jnp.concatenate([place(g_x[TAPS], DI, C), g_b[TAPS]], 0)
    smalls = lax.psum(
        (
            grad_pre, conv_w, conv_b, place(g_h[0, :Hl], H, Hl), place(g_h[1, :Hl], H, Hl),
            place(g_h[2, :Hl], H, Hl), place(g_gain[0], DI, C),
        ),
        ("seq", "fsdp"),
    )
    return (output[None], input_grad[None], g_in, g_out) + tuple(smalls)


def solution(mesh):
    seq, row, rep = P("fsdp", "seq", None), P("fsdp", None), P()
    in_specs = (seq, row, rep, row, rep, rep, rep, rep, rep, rep, row, seq)
    out_specs = (seq, seq, row, row) + (rep,) * 7
    return jax.shard_map(shards, mesh=mesh, in_specs=in_specs, out_specs=out_specs, check_vma=False)
```

```python
import functools

import jax
import jax.numpy as jnp
from jax import lax
from jax.experimental import pallas as pl
from jax.experimental.pallas import tpu as pltpu
from jax.sharding import PartitionSpec as P

P_SIZE = 64
N = 128
TAPS = 4
HALO = TAPS - 1
EDGE = 8
LANES = 128
EPSILON = 1e-05
F32 = jnp.float32
BF16 = jnp.bfloat16
MESH = pl.DeviceIdType.MESH
ANY = pl.BlockSpec(memory_space=pl.ANY)
VMEM = pl.BlockSpec(memory_space=pltpu.VMEM)
VMEM_BYTES = 56 << 20


def half(value):
    return value.astype(BF16)


def mm(left, right, dims):
    return lax.dot_general(half(left), half(right), (dims, ((), ())), preferred_element_type=F32)


NN = ((1,), (0,))
NT = ((1,), (1,))
TN = ((0,), (0,))


def split_dot(value, table, dims):
    top = half(value)
    rest = half(value - top.astype(F32))
    return mm(top, table, dims) + mm(rest, table, dims)


def head_table(channels):
    row = lax.broadcasted_iota(jnp.int32, (LANES, channels), 0)
    col = lax.broadcasted_iota(jnp.int32, (LANES, channels), 1)
    low = row * P_SIZE
    return half(((col >= low) & (col < low + P_SIZE)).astype(F32))


def triangle(length, lower):
    row = lax.broadcasted_iota(jnp.int32, (length, length), 0)
    col = lax.broadcasted_iota(jnp.int32, (length, length), 1)
    return half(((row >= col) if lower else (row <= col)).astype(F32))


def running_sum(values, lower):
    table = triangle(values.shape[0], lower)
    a = half(values)
    rest = values - a.astype(F32)
    b = half(rest)
    c = half(rest - b.astype(F32))
    return mm(table, a, NN) + mm(table, b, NN) + mm(table, c, NN)


def softplus(value):
    return jnp.maximum(value, 0.0) + jnp.log1p(jnp.exp(-jnp.abs(value)))


def params(**more):
    return pltpu.CompilerParams(vmem_limit_bytes=VMEM_BYTES, **more)


def meet(targets):
    barrier = pltpu.get_barrier_semaphore()
    for target in targets:
        pl.semaphore_signal(barrier, inc=1, device_id=target, device_id_type=MESH)
    pl.semaphore_wait(barrier, len(targets))


def remote(src, dst, send, recv, target):
    return pltpu.make_async_remote_copy(
        src_ref=src, dst_ref=dst, send_sem=send, recv_sem=recv, device_id=target, device_id_type=MESH
    )


def place():
    return lax.axis_index("seq"), lax.axis_index("fsdp")


def gather_kernel(n_s, n_f, C, DI, tok, seg, w, tok_all, seg_all, w_all, edge, edge_own, b_tok, b_w, b_seg, snd, rcv, loc):
    s, f = place()
    L = tok.shape[0]
    tail = w.shape[0] - 2 * DI
    right, left = lax.rem(s + 1, n_s), lax.rem(s + n_s - 1, n_s)
    parity = lax.rem(s, 2)
    pair = s + 1 - 2 * parity
    peers = [lax.rem(f + k, n_f) for k in range(1, n_f)]
    meet([(right, f), (left, f)] + [(s, p) for p in peers])
    count = [0]

    def go(src, dst, target):
        i = count[0]
        count[0] = i + 1
        copy = remote(src, dst, snd.at[i], rcv.at[i], target)
        copy.start()
        return copy

    def part(base, width):
        start = base + parity * (width // 2)
        return pl.ds(pl.multiple_of(start, 8), width // 2)

    first = go(tok.at[pl.ds(L - EDGE, EDGE)], edge_own, (right, f))
    started = []
    for p in peers:
        started.append(go(seg, seg_all.at[f], (s, p)))
        started.append(go(tok, tok_all.at[f], (s, p)))
    w_copies = []
    spots = (part(0, C), part(C, C), part(2 * C, tail))
    for p in peers:
        sources = (part(p * C, C), part(DI + p * C, C), part(2 * DI, tail))
        w_copies.append([go(w.at[a], w_all.at[f, b], (s, p)) for a, b in zip(sources, spots)])
    mine = [
        (tok, b_tok),
        (seg, b_seg),
        (w.at[pl.ds(pl.multiple_of(f * C, 8), C)], b_w.at[pl.ds(0, C)]),
        (w.at[pl.ds(pl.multiple_of(DI + f * C, 8), C)], b_w.at[pl.ds(C, C)]),
        (w.at[pl.ds(2 * DI, tail)], b_w.at[pl.ds(2 * C, tail)]),
    ]
    ins = [pltpu.make_async_copy(a, b, loc.at[i]) for i, (a, b) in enumerate(mine)]
    for c in ins:
        c.start()
    first.wait()
    edges = [go(edge_own, edge.at[f], (s, p)) for p in peers]
    outs = [pltpu.make_async_copy(edge_own, edge.at[f], loc.at[5])]
    outs[0].start()
    for c in ins:
        c.wait()
    for i, (a, b) in enumerate(((b_tok, tok_all.at[f]), (b_seg, seg_all.at[f]), (b_w, w_all.at[f]))):
        out = pltpu.make_async_copy(a, b, loc.at[6 + i])
        out.start()
        outs.append(out)
    relays = []
    for k, copies in enumerate(w_copies):
        source = lax.rem(f + n_f - (k + 1), n_f)
        for copy, spot in zip(copies, spots):
            copy.wait_recv()
            relays.append(go(w_all.at[source, spot], w_all.at[source, spot], (pair, f)))
    for copy in relays:
        copy.wait()
    for copies in w_copies:
        for copy in copies:
            copy.wait_send()
    for copy in started + edges:
        copy.wait()
    for out in outs:
        out.wait()


def gather(tok, seg, w, C, DI, n_s, n_f):
    L, D = tok.shape
    R = w.shape[1]
    own = 2 * C + w.shape[0] - 2 * DI
    sems = 1 + 9 * (n_f - 1)
    outs = [
        jax.ShapeDtypeStruct((n_f, L, D), BF16),
        jax.ShapeDtypeStruct((n_f,) + seg.shape, seg.dtype),
        jax.ShapeDtypeStruct((n_f, own, R), BF16),
        jax.ShapeDtypeStruct((n_f, EDGE, D), BF16),
        jax.ShapeDtypeStruct((EDGE, D), BF16),
    ]
    return pl.pallas_call(
        functools.partial(gather_kernel, n_s, n_f, C, DI),
        name="gather",
        out_shape=outs,
        in_specs=[ANY] * 3,
        out_specs=[ANY] * 5,
        scratch_shapes=[
            pltpu.VMEM((L, D), BF16),
            pltpu.VMEM((own, R), BF16),
            pltpu.VMEM(seg.shape, seg.dtype),
            pltpu.SemaphoreType.DMA((sems,)),
            pltpu.SemaphoreType.DMA((sems,)),
            pltpu.SemaphoreType.DMA((9,)),
        ],
        compiler_params=params(collective_id=0, has_side_effects=True),
    )(tok, seg, w)


def chain_steps(n_s, forward, state, through, result, out, snd, rcv):
    s, f = place()
    right, left = lax.rem(s + 1, n_s), lax.rem(s + n_s - 1, n_s)
    target = right if forward else left
    first = s == (0 if forward else n_s - 1)
    last = s == (n_s - 1 if forward else 0)
    copies = [remote(out.at[q], result.at[q], snd.at[q], rcv.at[q], (target, f)) for q in range(state.shape[0])]

    def start():
        @pl.when(first)
        def _():
            for q, copy in enumerate(copies):
                result[q] = jnp.zeros_like(result[q])
                out[q] = half(state[q])
                copy.start()

    def finish():
        @pl.when(jnp.logical_not(first))
        def _():
            for q, copy in enumerate(copies):
                copy.wait_recv()

                @pl.when(jnp.logical_not(last))
                def _():
                    out[q] = half(state[q] + result[q].astype(F32) * through[q, 0:1, :])
                    copy.start()

        @pl.when(jnp.logical_not(last))
        def _():
            for copy in copies:
                copy.wait_send()

    return [(right, f), (left, f)], start, finish


def chain_kernel(n_s, forward, state, through, result, out, snd, rcv):
    near, start, finish = chain_steps(n_s, forward, state, through, result, out, snd, rcv)
    meet(near)
    start()
    finish()


def chain_scratch(states):
    return [
        pltpu.VMEM(states.shape, BF16),
        pltpu.SemaphoreType.DMA((states.shape[0],)),
        pltpu.SemaphoreType.DMA((states.shape[0],)),
    ]


def chain(states, through, n_s):
    return pl.pallas_call(
        functools.partial(chain_kernel, n_s, True),
        name="chain_on",
        out_shape=jax.ShapeDtypeStruct(states.shape, BF16),
        in_specs=[VMEM] * 2,
        out_specs=VMEM,
        scratch_shapes=chain_scratch(states),
        compiler_params=params(collective_id=1, has_side_effects=True),
    )(states, through)


def slab_steps(n_f, product, sent, got, own, snd, rcv):
    s, f = place()

    def copy(k):
        return remote(sent.at[k - 1], got.at[k - 1], snd.at[k - 1], rcv.at[k - 1], (s, lax.rem(f + k, n_f)))

    def start():
        def step(k, carry):
            slab = product(lax.rem(f + k, n_f))

            @pl.when(k < n_f)
            def _():
                sent[k - 1] = half(slab)
                copy(k).start()

            @pl.when(k == n_f)
            def _():
                own[...] = slab

            return carry

        lax.fori_loop(1, n_f + 1, step, 0)

    def finish():
        total = own[...]
        for k in range(1, n_f):
            copy(k).wait()
            total = total + got[k - 1].astype(F32)
        return total

    return [(s, lax.rem(f + k, n_f)) for k in range(1, n_f)], start, finish


def slab_scratch(n_f, L, D):
    return [
        pltpu.VMEM((n_f - 1, L, D), BF16),
        pltpu.VMEM((n_f - 1, L, D), BF16),
        pltpu.VMEM((L, D), F32),
        pltpu.SemaphoreType.DMA((n_f - 1,)),
        pltpu.SemaphoreType.DMA((n_f - 1,)),
    ]


def out_kernel(n_s, n_f, state, through, ngate, w_out, tok, result, output, c_out, c_snd, c_rcv, sent, got, own, snd, rcv):
    near, chain_start, chain_finish = chain_steps(n_s, False, state, through, result, c_out, c_snd, c_rcv)

    def product(q):
        return mm(ngate[q], w_out[...], NN)

    peers, start, finish = slab_steps(n_f, product, sent, got, own, snd, rcv)
    meet(near + peers)
    chain_start()
    start()
    chain_finish()
    output[...] = half(tok[...].astype(F32) + finish())


def chain_and_out(states, through, ngate, w_out, tok, n_s, n_f):
    L, D = tok.shape
    return pl.pallas_call(
        functools.partial(out_kernel, n_s, n_f),
        name="chain_back",
        out_shape=[jax.ShapeDtypeStruct(states.shape, BF16), jax.ShapeDtypeStruct((L, D), BF16)],
        in_specs=[VMEM] * 5,
        out_specs=[VMEM] * 2,
        scratch_shapes=chain_scratch(states) + slab_scratch(n_f, L, D),
        compiler_params=params(collective_id=2, has_side_effects=True),
    )(states, through, ngate, w_out, tok)


def input_kernel(n_f, dz, dx, dbd, w, tok, cot, gain, grad, g_pre, sent, got, own, snd, rcv):
    C = dz.shape[2]

    def product(q):
        blocks = []
        for j in range(n_f):
            block = mm(dz[q], w[j, 0:C, :], NN) + mm(dx[q], w[j, C : 2 * C, :], NN)
            blocks.append(block + mm(dbd[q], w[j, 2 * C :, :], NN))
        return jnp.concatenate(blocks, 1)

    peers, start, finish = slab_steps(n_f, product, sent, got, own, snd, rcv)
    meet(peers)
    start()
    tokf = tok[...].astype(F32)
    inv = lax.rsqrt(jnp.mean(tokf * tokf, 1, keepdims=True) + EPSILON)
    scaled = tokf * inv
    gn = finish()
    g_pre[...] = jnp.broadcast_to(jnp.sum(gn * scaled, 0, keepdims=True), g_pre.shape)
    weighted = gn * gain[...]
    grad[...] = half(
        cot[...].astype(F32) + inv * (weighted - scaled * jnp.mean(weighted * scaled, 1, keepdims=True))
    )


def input_grads(dz, dx, dbd, w, tok, cot, gain, n_f):
    L, D = tok.shape
    return pl.pallas_call(
        functools.partial(input_kernel, n_f),
        name="input_grads",
        out_shape=[jax.ShapeDtypeStruct((L, D), BF16), jax.ShapeDtypeStruct((8, D), F32)],
        in_specs=[VMEM] * 7,
        out_specs=[VMEM] * 2,
        scratch_shapes=slab_scratch(n_f, L, D),
        compiler_params=params(collective_id=4, has_side_effects=True),
    )(dz, dx, dbd, w, tok, cot, gain)


def total_kernel(n_f, part, total, got, snd, rcv):
    s, f = place()
    peers = [lax.rem(f + k, n_f) for k in range(1, n_f)]
    meet([(s, p) for p in peers])
    copies = []
    for k, p in enumerate(peers):
        copy = remote(part, got.at[k], snd.at[k], rcv.at[k], (s, p))
        copy.start()
        copies.append(copy)
    value = part[...]
    for k, copy in enumerate(copies):
        copy.wait()
        value = value + got[k]
    total[...] = value


def total_over_fsdp(part, n_f):
    return pl.pallas_call(
        functools.partial(total_kernel, n_f),
        name="total",
        out_shape=jax.ShapeDtypeStruct(part.shape, F32),
        in_specs=[VMEM],
        out_specs=VMEM,
        scratch_shapes=[
            pltpu.VMEM((n_f - 1,) + part.shape, F32),
            pltpu.SemaphoreType.DMA((n_f - 1,)),
            pltpu.SemaphoreType.DMA((n_f - 1,)),
        ],
        compiler_params=params(collective_id=3, has_side_effects=True),
    )(part)


def small_rows(C, D, pair):
    return 8 * C // LANES, 8, 8 * pair // LANES, -(-(D // LANES) // 8) * 8


def small_kernel(n_s, n_f, g_x, g_gain, g_h, g_b, g_pre, everything, buf, got, snd, rcv, f_snd, f_rcv):
    s, f = place()
    C, D, pair = g_x.shape[1], g_pre.shape[1], g_b.shape[1]
    counts = small_rows(C, D, pair)
    levels = n_s.bit_length() - 1

    def flip(k):
        bit = 1 << k
        return s + bit - 2 * bit * lax.rem(s // bit, 2)

    meet([(flip(k), f) for k in range(levels)] + [(s, lax.rem(f + k, n_f)) for k in range(1, n_f)])
    row = lax.broadcasted_iota(jnp.int32, (8, LANES), 0)
    for j in range(C // LANES):
        lanes = slice(j * LANES, (j + 1) * LANES)
        buf[0, 8 * j : 8 * j + 8, :] = jnp.where(row == TAPS + 1, g_gain[:, lanes], g_x[:, lanes])
    at = counts[0]
    buf[0, at : at + 8, :] = g_h[...]
    at += 8
    for j in range(pair // LANES):
        buf[0, at + 8 * j : at + 8 * j + 8, :] = g_b[:, j * LANES : (j + 1) * LANES]
    at += counts[2]
    for j in range(D // LANES):
        buf[0, at + j : at + j + 1, :] = g_pre[0:1, j * LANES : (j + 1) * LANES]
    for j in range(D // LANES, counts[3]):
        buf[0, at + j : at + j + 1, :] = jnp.zeros((1, LANES), F32)
    for k in range(levels):
        copy = remote(buf.at[k], got.at[k], snd.at[k], rcv.at[k], (flip(k), f))
        copy.start()
        copy.wait()
        buf[k + 1] = buf[k] + got[k]
    everything[f] = buf[levels]
    copies = []
    for k in range(1, n_f):
        target = (s, lax.rem(f + k, n_f))
        copy = remote(buf.at[levels], everything.at[f], f_snd.at[k - 1], f_rcv.at[k - 1], target)
        copy.start()
        copies.append(copy)
    for copy in copies:
        copy.wait()


def spread_small_kernel(n_f, DI, D, everything, conv_w, conv_b, gain, pre, heads):
    pair = conv_w.shape[1] - DI
    C = DI // n_f
    counts = small_rows(C, D, pair)
    for f in range(n_f):
        for j in range(C // LANES):
            lanes = slice(f * C + j * LANES, f * C + (j + 1) * LANES)
            conv_w[:, lanes] = everything[f, 8 * j : 8 * j + TAPS, :]
            conv_b[:, lanes] = everything[f, 8 * j + TAPS : 8 * j + TAPS + 1, :]
            gain[:, lanes] = everything[f, 8 * j + TAPS + 1 : 8 * j + TAPS + 2, :]
        heads[f] = everything[f, counts[0] : counts[0] + 8, :]
    at = counts[0] + 8
    both = everything[0, at:, :]
    for f in range(1, n_f):
        both = both + everything[f, at:, :]
    for j in range(pair // LANES):
        lanes = slice(DI + j * LANES, DI + (j + 1) * LANES)
        conv_w[:, lanes] = both[8 * j : 8 * j + TAPS]
        conv_b[:, lanes] = both[8 * j + TAPS : 8 * j + TAPS + 1]
    for j in range(D // LANES):
        pre[:, j * LANES : (j + 1) * LANES] = both[counts[2] + j : counts[2] + j + 1]


def small_sums(g_x, g_gain, g_h, g_b, g_pre, n_s, n_f):
    C, D, pair = g_x.shape[1], g_pre.shape[1], g_b.shape[1]
    rows = sum(small_rows(C, D, pair))
    levels = n_s.bit_length() - 1
    DI = C * n_f
    everything = pl.pallas_call(
        functools.partial(small_kernel, n_s, n_f),
        name="small",
        out_shape=jax.ShapeDtypeStruct((n_f, rows, LANES), F32),
        in_specs=[VMEM] * 5,
        out_specs=VMEM,
        scratch_shapes=[
            pltpu.VMEM((levels + 1, rows, LANES), F32),
            pltpu.VMEM((levels, rows, LANES), F32),
            pltpu.SemaphoreType.DMA((levels,)),
            pltpu.SemaphoreType.DMA((levels,)),
            pltpu.SemaphoreType.DMA((n_f - 1,)),
            pltpu.SemaphoreType.DMA((n_f - 1,)),
        ],
        compiler_params=params(collective_id=5, has_side_effects=True),
    )(g_x, g_gain, g_h, g_b, g_pre)
    return pl.pallas_call(
        functools.partial(spread_small_kernel, n_f, DI, D),
        name="spread_small",
        out_shape=[
            jax.ShapeDtypeStruct((TAPS, DI + pair), F32),
            jax.ShapeDtypeStruct((1, DI + pair), F32),
            jax.ShapeDtypeStruct((1, DI), F32),
            jax.ShapeDtypeStruct((1, D), F32),
            jax.ShapeDtypeStruct((n_f, 8, LANES), F32),
        ],
        in_specs=[VMEM],
        out_specs=[VMEM] * 5,
    )(everything)


def fill(scratch, halo, raw):
    length = raw.shape[0]
    scratch[0:EDGE, :] = halo.astype(F32)
    scratch[EDGE : EDGE + length, :] = raw.astype(F32)


def conv(scratch, length, kernel, bias, cols):
    pre = bias[...] + kernel[HALO : HALO + 1, :] * scratch[EDGE : EDGE + length, :]
    for k in range(HALO):
        start = EDGE - HALO + k
        pre = pre + kernel[k : k + 1, :] * (scratch[start : start + length, :] * cols[:, k : k + 1])
    return pre


def silu(value):
    return value * jax.nn.sigmoid(value)


def head_rows(values, pick):
    a = half(values)
    rest = values - a.astype(F32)
    b = half(rest)
    c = half(rest - b.astype(F32))
    rows = mm(a, pick, NN) + mm(b, pick, NN) + mm(c, pick, NN)
    used = jnp.sum(pick.astype(F32), 0, keepdims=True)
    return rows[0:1, :] + 100.0 * (used - 1.0), jnp.exp(rows[1:2, :]), rows[2:3, :]


def marks_of(seg, before, s):
    L = seg.shape[1]
    before = jnp.where(s > 0, before, -1)
    both = jnp.concatenate([before, seg], 1)
    rows = [(both[:, L - k : 2 * L - k] == seg).astype(F32) for k in range(HALO, 0, -1)]
    rows.append((seg == seg[:, L - 1 : L]).astype(F32))
    rows.append((seg == before[:, L - 1 : L]).astype(F32))
    rows.append(seg.astype(F32))
    return jnp.concatenate(rows + [jnp.zeros((LANES - len(rows), L), F32)], 0)


def front_kernel(
    where, tok, edge, w, pre_gain, seg, before, pick, hv, kw_x, kb_x, kw_b, kb_b,
    z, x, x_halo, b, b_halo, d, normed, cols, seg_row, state, through, pre_x, xd, pre_b, bc, cum, cum_row, s_x, s_b,
):
    L, C = x.shape
    n_f, _, R = w.shape
    tokf = jnp.concatenate([edge[...], tok[...]], 0).astype(F32)
    inv = lax.rsqrt(jnp.mean(tokf * tokf, 1, keepdims=True) + EPSILON)
    n = half(tokf * inv * pre_gain[...])
    acc = mm(n[:, 0:R], w[0], NT)
    normed[0] = n[EDGE:, 0:R]
    for j in range(1, n_f):
        acc = acc + mm(n[:, j * R : (j + 1) * R], w[j], NT)
        normed[j] = n[EDGE:, j * R : (j + 1) * R]
    p = half(acc)
    z[...] = p[EDGE:, 0:C]
    x[...] = p[EDGE:, C : 2 * C]
    b[...] = p[EDGE:, 2 * C : 2 * C + 2 * N]
    inside = where[1] > 0
    pe = p[0:EDGE, :].astype(F32)
    pe = half(jnp.where(inside, pe, 0.0))
    x_halo[...] = pe[:, C : 2 * C]
    b_halo[...] = pe[:, 2 * C : 2 * C + 2 * N]
    d[...] = half(mm(p[EDGE:, 2 * C + 2 * N :], pick[...], NN))

    table = head_table(C)
    m = marks_of(seg[...], before[...], where[1])
    seg_row[...] = jnp.broadcast_to(m[5:6, :], seg_row.shape)
    c = jnp.transpose(m)
    cols[...] = c
    fill(s_x, x_halo[...], x[...])
    fill(s_b, b_halo[...], b[...])
    px = conv(s_x, L, kw_x, kb_x, c)
    pb = conv(s_b, L, kw_b, kb_b, c)
    pre_x[...] = px
    pre_b[...] = pb
    bc[...] = half(silu(pb))
    bias, decay, _ = head_rows(hv[...], pick[...])
    step = softplus(d[...].astype(F32) + bias)
    rate = -step * decay
    total = running_sum(rate, True)
    cum[...] = total
    cum_row[...] = jnp.transpose(total)[0 : cum_row.shape[0], :]
    last = total[L - 1 : L, :]
    to_end = jnp.exp(last - total) * c[:, 3:4]
    entry_last = jnp.exp(last) * c[L - 1 : L, 4:5]
    through[...] = split_dot(jnp.broadcast_to(entry_last, (8, LANES)), table, NN)
    xdv = split_dot(step, table, NN) * silu(px)
    xd[...] = half(xdv)
    wx = half(split_dot(to_end, table, NN) * xdv)
    state[...] = mm(bc[:, 0:N], wx, TN)


def block_rows(L):
    return min(L, 128)


def live_rows(cols, seg_row, r, rows, width):
    row = lax.broadcasted_iota(jnp.int32, (rows, width), 0) + r * rows
    col = lax.broadcasted_iota(jnp.int32, (rows, width), 1)
    same = cols[r * rows : (r + 1) * rows, 5:6] == seg_row[0:1, 0:width]
    return (row >= col) & same


def mix_kernel(where, pre_x, xd, bc, cum, cum_row, cols, seg_row, enter, z, gg, gain, pick, hv, plain, mixed, sums):
    L, C = xd.shape
    rows = block_rows(L)
    table = head_table(C)
    cv = cum[...]
    entry = jnp.exp(cv) * cols[:, 4:5]
    carried = mm(bc[:, N : 2 * N], enter[...], NN) * split_dot(entry, table, NN)
    for r in range(L // rows):
        width = (r + 1) * rows
        mine = slice(r * rows, (r + 1) * rows)
        scores = jnp.where(
            live_rows(cols, seg_row, r, rows, width), mm(bc[mine, N : 2 * N], bc[0:width, 0:N], NT), 0.0
        )
        for h in range(0, C // P_SIZE, 2):
            pieces = []
            for g in (h, h + 1):
                gap = jnp.minimum(cum[mine, g : g + 1] - cum_row[g : g + 1, 0:width], 0.0)
                pieces.append(mm(scores * jnp.exp(gap), xd[0:width, g * P_SIZE : (g + 1) * P_SIZE], NN))
            plain[mine, h * P_SIZE : (h + 2) * P_SIZE] = jnp.concatenate(pieces, 1)
    y = plain[...] + carried
    plain[...] = y
    skip = head_rows(hv[...], pick[...])[2]
    skip = split_dot(jnp.broadcast_to(skip, (8, LANES)), table, NN)[0:1, :]
    m = half(y + skip * silu(pre_x[...]))
    mixed[...] = m
    gated = m.astype(F32) * silu(z[...].astype(F32))
    sg = gg[...].astype(F32) * gain[...]
    one = jnp.sum(gated * gated, 1, keepdims=True)
    two = jnp.sum(sg * gated, 1, keepdims=True)
    lane = lax.broadcasted_iota(jnp.int32, (L, LANES), 1)
    both = jnp.where(lane == 0, one, jnp.where(lane == 1, two, 0.0))
    sums[...] = jnp.transpose(both)[0:8, :]


def gate_kernel(DI, where, mixed, z, gg, gain, total, cum, cols, bc, ngate, dz, dy, d_enter, d_gain):
    L, C = mixed.shape
    table = head_table(C)
    sums = jnp.transpose(jnp.concatenate([total[...], jnp.zeros((LANES - 8, L), F32)], 0))
    inv = lax.rsqrt(sums[:, 0:1] / DI + EPSILON)
    inner = inv * (sums[:, 1:2] / DI)
    y = mixed[...].astype(F32)
    zf = z[...].astype(F32)
    sig = jax.nn.sigmoid(zf)
    gz = zf * sig
    unit = y * gz * inv
    g = gg[...].astype(F32)
    ngate[...] = half(unit * gain[...])

    @pl.when(pl.program_id(0) == 0)
    def _():
        d_gain[...] = jnp.zeros_like(d_gain)

    d_gain[...] += jnp.broadcast_to(jnp.sum(g * unit, 0, keepdims=True), d_gain.shape)
    grad = inv * (g * gain[...] - unit * inner)
    d = half(grad * gz)
    dy[...] = d
    dz[...] = half(grad * y * sig * (1.0 + zf * (1.0 - sig)))
    entry = jnp.exp(cum[...]) * cols[:, 4:5]
    edy = half(split_dot(entry, table, NN) * d.astype(F32))
    d_enter[...] = mm(bc[:, N : 2 * N], edy, TN)


def silu_grad(pre, sigma):
    return sigma * (1.0 + pre * (1.0 - sigma))


def conv_back(dpre, raw, halo, kernel, cols, s_raw, s_grad, grads):
    length = dpre.shape[0]
    fill(s_raw, halo, raw)
    grads[TAPS : TAPS + 1, :] += jnp.sum(dpre, 0, keepdims=True)
    grads[HALO : HALO + 1, :] += jnp.sum(dpre * s_raw[EDGE : EDGE + length, :], 0, keepdims=True)
    d_raw = kernel[HALO : HALO + 1, :] * dpre
    width = dpre.shape[1]
    d_halo = jnp.zeros((EDGE, width), F32)
    s_grad[0:EDGE, :] = jnp.zeros((EDGE, width), F32)
    s_grad[EDGE + length : EDGE + length + EDGE, :] = jnp.zeros((EDGE, width), F32)
    for k in range(HALO):
        masked = dpre * cols[:, k : k + 1]
        start = EDGE - HALO + k
        grads[k : k + 1, :] += jnp.sum(masked * s_raw[start : start + length, :], 0, keepdims=True)
        s_grad[EDGE : EDGE + length, :] = masked
        up = HALO - k
        d_raw = d_raw + kernel[k : k + 1, :] * s_grad[EDGE + up : EDGE + up + length, :]
        d_halo = d_halo + kernel[k : k + 1, :] * s_grad[up : up + EDGE, :]
    return d_raw, d_halo


def back_kernel(
    where, x, x_halo, b, b_halo, d, cols, seg_row, k_x, k_b, pick, hv, pre_x, xd, pre_b, bc, cum, cum_row, enter, grad, plain, dy,
    dx, dbd, tail, halo, g_x, g_b, g_h, s_x, s_gx, s_b, s_gb, s_dxd, s_ds,
):
    L, C = xd.shape
    rows = block_rows(L)
    table = head_table(C)
    c = cols[...]
    cv = cum[...]
    bias, decay_rate, skip = head_rows(hv[...], pick[...])

    @pl.when(pl.program_id(0) == 0)
    def _():
        g_x[...] = jnp.zeros_like(g_x)
        g_b[...] = jnp.zeros_like(g_b)
        g_h[...] = jnp.zeros_like(g_h)

    s_dxd[...] = jnp.zeros_like(s_dxd)
    s_ds[...] = jnp.zeros_like(s_ds)
    for r in range(L // rows):
        width = (r + 1) * rows
        mine = slice(r * rows, (r + 1) * rows)
        live = live_rows(cols, seg_row, r, rows, width)
        scores = jnp.where(live, mm(bc[mine, N : 2 * N], bc[0:width, 0:N], NT), 0.0)
        d_scores = jnp.zeros((rows, width), F32)
        for h in range(0, C // P_SIZE, 2):
            pieces = []
            for g in (h, h + 1):
                lanes = slice(g * P_SIZE, (g + 1) * P_SIZE)
                decay = jnp.exp(jnp.minimum(cum[mine, g : g + 1] - cum_row[g : g + 1, 0:width], 0.0))
                pieces.append(mm(scores * decay, dy[mine, lanes], TN))
                d_scores = d_scores + mm(dy[mine, lanes], xd[0:width, lanes], NT) * decay
            s_dxd[0:width, h * P_SIZE : (h + 2) * P_SIZE] += jnp.concatenate(pieces, 1)
        s_ds[mine, 0:width] = jnp.where(live, d_scores, 0.0)
    ds = half(s_ds[...])
    last = cv[L - 1 : L, :]
    to_end = split_dot(jnp.exp(last - cv) * c[:, 3:4], table, NN)
    entry = split_dot(jnp.exp(cv) * c[:, 4:5], table, NN)
    dyf = dy[...].astype(F32)
    xdf = xd[...].astype(F32)
    dwx = mm(bc[:, 0:N], grad[...], NN)
    wx = half(to_end * xdf)
    d_b = mm(wx, grad[...], NT) + mm(ds, bc[:, N : 2 * N], TN)
    d_c = mm(half(entry * dyf), enter[...], NT) + mm(ds, bc[:, 0:N], NN)
    u = split_dot(wx.astype(F32) * dwx, table, NT)
    dxd_in = s_dxd[...]
    dcum = split_dot(dyf * plain[...] - xdf * dxd_in, table, NT) - u
    carry = jnp.sum(enter[...].astype(F32) * grad[...].astype(F32), 0, keepdims=True)
    carry = split_dot(jnp.broadcast_to(carry, (8, C)), table, NT)[0:1, :]
    at_last = jnp.sum(u, 0, keepdims=True) + jnp.exp(last) * c[L - 1 : L, 4:5] * carry
    row = lax.broadcasted_iota(jnp.int32, (L, LANES), 0)
    dcum = dcum + jnp.where(row == L - 1, at_last, 0.0)
    drate = running_sum(dcum, False)
    px = pre_x[...]
    sig = jax.nn.sigmoid(px)
    xf = px * sig
    dxd = dxd_in + to_end * dwx
    raw_step = d[...].astype(F32) + bias
    step = softplus(raw_step)
    ddt = split_dot(xf * dxd, table, NT) - drate * decay_rate
    ddt_raw = ddt * jax.nn.sigmoid(raw_step)
    dbd[:, 2 * N :] = half(mm(ddt_raw, pick[...], NT))
    g_h[0:1, :] += jnp.sum(ddt_raw, 0, keepdims=True)
    g_h[1:2, :] += jnp.sum(drate * (-step * decay_rate), 0, keepdims=True)
    g_h[2:3, :] += split_dot(jnp.broadcast_to(jnp.sum(dyf * xf, 0, keepdims=True), (8, C)), table, NT)[0:1, :]
    skip = split_dot(jnp.broadcast_to(skip, (8, LANES)), table, NN)[0:1, :]
    d_x = split_dot(step, table, NN) * dxd + skip * dyf
    rx, hx = conv_back(d_x * silu_grad(px, sig), x[...], x_halo[...], k_x, c, s_x, s_gx, g_x)
    pb = pre_b[...]
    d_bc = jnp.concatenate([d_b, d_c], 1) * silu_grad(pb, jax.nn.sigmoid(pb))
    rb, hb = conv_back(d_bc, b[...], b_halo[...], k_b, c, s_b, s_gb, g_b)
    dx[...] = half(rx)
    dbd[:, 0 : 2 * N] = half(rb)
    tail[:, 0:C] = rx[L - EDGE : L, :]
    tail[:, C : C + 2 * N] = rb[L - EDGE : L, :]
    halo[:, 0:C] = half(hx)
    halo[:, C : C + 2 * N] = half(hb)


def weight_kernel(where, dx, normed, out, flipped):
    n_f, L, W = dx.shape

    @pl.when(pl.program_id(0) == 0)
    def _():
        for q in range(n_f):
            flipped[:, q * L : (q + 1) * L] = jnp.transpose(dx[q])

    out[...] = half(mm(flipped[...], normed[...].reshape(n_f * L, normed.shape[-1]), NN))


def weight_grads(where, dx, normed):
    n_f, L, W = dx.shape
    R = normed.shape[-1]
    return pl.pallas_call(
        weight_kernel,
        name="weight_grads",
        grid_spec=pltpu.PrefetchScalarGridSpec(
            num_scalar_prefetch=1,
            grid=(n_f,),
            in_specs=[
                pl.BlockSpec((n_f, L, W), lambda k, p: (0, 0, 0)),
                pl.BlockSpec((n_f, None, L, R), lambda k, p: (0, k, 0, 0)),
            ],
            out_specs=pl.BlockSpec((None, W, R), lambda k, p: (k, 0, 0)),
            scratch_shapes=[pltpu.VMEM((W, n_f * L), BF16)],
        ),
        out_shape=jax.ShapeDtypeStruct((n_f, W, R), BF16),
        compiler_params=params(dimension_semantics=("arbitrary",)),
        cost_estimate=pl.CostEstimate(flops=2 * n_f * L * W * R * n_f, bytes_accessed=4 * n_f * W * R, transcendentals=0),
    )(where, dx, normed)


def per(*shape, col=0):
    return pl.BlockSpec((None,) + shape, lambda q, p: (q, 0, col))


def fixed(*shape):
    return pl.BlockSpec(shape, lambda q, p: (0,) * len(shape))


def mine(*shape):
    return pl.BlockSpec(shape, lambda q, p: (0, p[0]))


def shaped(*shape, dtype=F32):
    return jax.ShapeDtypeStruct(shape, dtype)


def shards(tokens, seg_ids, pre_gain, w_in, conv_weight, conv_bias, dt_bias, a_log, d_skip, norm_gain, w_out, cotangent):
    n_s = lax.axis_size("seq")
    n_f = lax.axis_size("fsdp")
    s = lax.axis_index("seq")
    f = lax.axis_index("fsdp")
    L, D = tokens.shape[1:]
    DI = norm_gain.shape[0]
    H = dt_bias.shape[0]
    Hl = H // n_f
    C = DI // n_f
    pair = conv_bias.shape[0] - DI
    T = n_f * L
    R = w_in.shape[0]
    W = 2 * C + pair + H
    HR = -(-Hl // 8) * 8

    where = jnp.stack([f, s]).astype(jnp.int32)
    pick = half((jnp.arange(H)[:, None] - f * Hl == jnp.arange(LANES)[None, :]) & (jnp.arange(LANES)[None, :] < Hl))
    hv = jnp.concatenate([dt_bias[None], a_log[None], d_skip[None], jnp.zeros((5, H), F32)], 0)
    gain = norm_gain[None]
    bias = conv_bias[None]
    pre = pre_gain[None]

    tok_all, seg_all, w_all, edge, _ = gather(tokens[0], seg_ids, w_in.T, C, DI, n_s, n_f)
    cot_own, _ = lax.optimization_barrier((cotangent[0], tok_all))
    cot_all = lax.all_gather(cot_own, "fsdp").reshape(T, D)

    big, small, lane, st = per(L, C), per(L, pair), per(L, LANES), per(N, C)
    row8, halo_x, halo_b, hr = per(8, L), per(EDGE, C), per(EDGE, pair), per(HR, L)
    kw_x, kb_x = mine(TAPS, C), mine(1, C)
    kw_b = pl.BlockSpec((TAPS, pair), lambda q, p: (0, DI // pair))
    kb_b = pl.BlockSpec((1, pair), lambda q, p: (0, DI // pair))
    pick_spec, hv_spec = fixed(H, LANES), fixed(8, H)

    def call(body, name, ins, outs, shapes, flops, scratch=()):
        return pl.pallas_call(
            body,
            name=name,
            grid_spec=pltpu.PrefetchScalarGridSpec(
                num_scalar_prefetch=1, grid=(n_f,), in_specs=ins, out_specs=outs, scratch_shapes=list(scratch)
            ),
            out_shape=shapes,
            compiler_params=params(dimension_semantics=("arbitrary",)),
            cost_estimate=pl.CostEstimate(flops=flops, bytes_accessed=20 * T * C, transcendentals=0),
        )

    z, x, x_halo, b, b_halo, d, normed, cols, seg_row, state, through, pre_x, xd, pre_b, bc, cum, cum_row = call(
        front_kernel,
        "front",
        [
            per(L, D), per(EDGE, D), fixed(n_f, W, R), fixed(1, D),
            pl.BlockSpec((None, 1, L), lambda q, p: (q, 0, p[1])),
            pl.BlockSpec((None, 1, L), lambda q, p: (q, 0, jnp.maximum(p[1] - 1, 0))),
            pick_spec, hv_spec, kw_x, kb_x, kw_b, kb_b,
        ],
        [
            big, big, halo_x, small, halo_b, lane, pl.BlockSpec((None, n_f, L, R), lambda q, p: (q, 0, 0, 0)), lane, row8,
            st, per(8, C), big, big, small, small, lane, hr,
        ],
        [
            shaped(n_f, L, C, dtype=BF16), shaped(n_f, L, C, dtype=BF16), shaped(n_f, EDGE, C, dtype=BF16),
            shaped(n_f, L, pair, dtype=BF16), shaped(n_f, EDGE, pair, dtype=BF16), shaped(n_f, L, LANES, dtype=BF16),
            shaped(n_f, n_f, L, R, dtype=BF16), shaped(n_f, L, LANES), shaped(n_f, 8, L),
            shaped(n_f, N, C), shaped(n_f, 8, C), shaped(n_f, L, C), shaped(n_f, L, C, dtype=BF16),
            shaped(n_f, L, pair), shaped(n_f, L, pair, dtype=BF16), shaped(n_f, L, LANES), shaped(n_f, HR, L),
        ],
        2 * T * D * W,
        [pltpu.VMEM((L + EDGE, C), F32), pltpu.VMEM((L + EDGE, pair), F32)],
    )(where, tok_all, edge, w_all, pre, seg_all, seg_all, pick, hv, conv_weight, bias, conv_weight, bias)
    enter = chain(state, through, n_s)
    ggate = half(lax.dot_general(cot_all, w_out, (NT, ((), ())), preferred_element_type=F32)).reshape(n_f, L, C)
    plain, mixed, sums = call(
        mix_kernel,
        "mix",
        [big, big, small, lane, hr, lane, row8, st, big, big, mine(1, C), pick_spec, hv_spec],
        [big, big, row8],
        [shaped(n_f, L, C), shaped(n_f, L, C, dtype=BF16), shaped(n_f, 8, L)],
        10 * T * D * C // 4,
    )(where, pre_x, xd, bc, cum, cum_row, cols, seg_row, enter, z, ggate, gain, pick, hv)
    total = total_over_fsdp(sums, n_f)
    ngate, dz, dy, d_enter, g_gain = call(
        functools.partial(gate_kernel, DI),
        "gate",
        [big, big, big, mine(1, C), row8, lane, lane, small],
        [big, big, big, st, fixed(8, C)],
        [shaped(n_f, L, C, dtype=BF16)] * 3 + [shaped(n_f, N, C), shaped(8, C)],
        T * D * C,
    )(where, mixed, z, ggate, gain, total, cum, cols, bc)
    g_out = half(lax.dot_general(ngate.reshape(T, C), cot_all, (TN, ((), ())), preferred_element_type=F32))
    gz = weight_grads(where, dz, normed)
    d_enter, g_out, gz = lax.optimization_barrier((d_enter, g_out, gz))
    g_out, gz = lax.psum((g_out, gz), "seq")
    grad, output = chain_and_out(d_enter, through, ngate, w_out, tokens[0], n_s, n_f)

    def exchange(value):
        return lax.all_to_all(value, "fsdp", 0, 0, tiled=True)

    dx, dbd, tail, halo, g_x, g_b, g_h = call(
        back_kernel,
        "back",
        [
            big, halo_x, small, halo_b, lane, lane, row8, kw_x, kw_b, pick_spec, hv_spec,
            big, big, small, small, lane, hr, st, st, big, big,
        ],
        [big, per(L, pair + H), per(EDGE, C + pair), per(EDGE, C + pair), fixed(8, C), fixed(8, pair), fixed(8, LANES)],
        [
            shaped(n_f, L, C, dtype=BF16), shaped(n_f, L, pair + H, dtype=BF16), shaped(n_f, EDGE, C + pair),
            shaped(n_f, EDGE, C + pair, dtype=BF16), shaped(8, C), shaped(8, pair), shaped(8, LANES),
        ],
        30 * T * D * C // 4,
        [
            pltpu.VMEM((L + EDGE, C), F32), pltpu.VMEM((L + 2 * EDGE, C), F32),
            pltpu.VMEM((L + EDGE, pair), F32), pltpu.VMEM((L + 2 * EDGE, pair), F32),
            pltpu.VMEM((L, C), F32), pltpu.VMEM((L, L), F32),
        ],
    )(where, x, x_halo, b, b_halo, d, cols, seg_row, conv_weight, conv_weight, pick, hv,
      pre_x, xd, pre_b, bc, cum, cum_row, enter, grad, plain, dy)
    got = lax.ppermute(halo, "seq", [(i + 1, i) for i in range(n_s - 1)])
    ends = half(tail + got.astype(F32))
    dx = lax.dynamic_update_slice(dx, ends[..., :C], (0, L - EDGE, 0))
    dbd = lax.dynamic_update_slice(dbd, ends[..., C:], (0, L - EDGE, 0))
    gx = exchange(jnp.concatenate([weight_grads(where, dx, normed), weight_grads(where, dbd, normed)], 1))
    gb = half(jnp.sum(gx[:, C:].astype(F32), 0))
    gx = gx[:, :C].reshape(DI, R)
    gx, gb, gz, g_out = lax.optimization_barrier((gx, gb, gz, g_out))
    gx, gb = lax.psum((gx, gb), "seq")
    gz = exchange(gz).reshape(DI, R)
    g_in = jnp.concatenate([gz, gx, gb], 0).astype(F32).T
    input_grad, g_pre = input_grads(dz, dx, dbd, w_all, tokens[0], cotangent[0], pre, n_f)
    conv_w, conv_b, g_gain, g_pre, g_h = small_sums(g_x, g_gain, g_h, g_b, g_pre, n_s, n_f)
    g_heads = [g_h[:, i, :Hl].reshape(H) for i in range(3)]
    return (output[None], input_grad[None], g_in, g_out.astype(F32), g_pre[0], conv_w, conv_b[0], *g_heads, g_gain[0])


def solution(mesh):
    seq, row, rep = P("fsdp", "seq", None), P("fsdp", None), P()
    in_specs = (seq, row, rep, row, rep, rep, rep, rep, rep, rep, row, seq)
    out_specs = (seq, seq, row, row) + (rep,) * 7
    return jax.shard_map(shards, mesh=mesh, in_specs=in_specs, out_specs=out_specs, check_vma=False)
```

```python
import functools

import jax
import jax.numpy as jnp
from jax import lax
from jax.experimental import pallas as pl
from jax.experimental.pallas import tpu as pltpu
from jax.sharding import PartitionSpec as P

P_SIZE = 64
N = 128
TAPS = 4
HALO = TAPS - 1
EDGE = 8
LANES = 128
EPSILON = 1e-05
F32 = jnp.float32
BF16 = jnp.bfloat16
MESH = pl.DeviceIdType.MESH
ANY = pl.BlockSpec(memory_space=pl.ANY)
VMEM = pl.BlockSpec(memory_space=pltpu.VMEM)
VMEM_BYTES = 56 << 20


def half(value):
    return value.astype(BF16)


def mm(left, right, dims):
    return lax.dot_general(half(left), half(right), (dims, ((), ())), preferred_element_type=F32)


NN = ((1,), (0,))
NT = ((1,), (1,))
TN = ((0,), (0,))


def split_dot(value, table, dims):
    top = half(value)
    rest = half(value - top.astype(F32))
    return mm(top, table, dims) + mm(rest, table, dims)


def head_table(channels):
    row = lax.broadcasted_iota(jnp.int32, (LANES, channels), 0)
    col = lax.broadcasted_iota(jnp.int32, (LANES, channels), 1)
    low = row * P_SIZE
    return half(((col >= low) & (col < low + P_SIZE)).astype(F32))


def triangle(length, lower):
    row = lax.broadcasted_iota(jnp.int32, (length, length), 0)
    col = lax.broadcasted_iota(jnp.int32, (length, length), 1)
    return half(((row >= col) if lower else (row <= col)).astype(F32))


def running_sum(values, lower):
    table = triangle(values.shape[0], lower)
    a = half(values)
    rest = values - a.astype(F32)
    b = half(rest)
    c = half(rest - b.astype(F32))
    return mm(table, a, NN) + mm(table, b, NN) + mm(table, c, NN)


def softplus(value):
    return jnp.maximum(value, 0.0) + jnp.log1p(jnp.exp(-jnp.abs(value)))


def params(**more):
    return pltpu.CompilerParams(vmem_limit_bytes=VMEM_BYTES, **more)


def meet(targets):
    barrier = pltpu.get_barrier_semaphore()
    for target in targets:
        pl.semaphore_signal(barrier, inc=1, device_id=target, device_id_type=MESH)
    pl.semaphore_wait(barrier, len(targets))


def remote(src, dst, send, recv, target):
    return pltpu.make_async_remote_copy(
        src_ref=src, dst_ref=dst, send_sem=send, recv_sem=recv, device_id=target, device_id_type=MESH
    )


def place():
    return lax.axis_index("seq"), lax.axis_index("fsdp")


class Fan:
    def __init__(self, src, dst, snd, rcv, n_f):
        s, f = place()
        self.square = n_f == 4
        rows = src.shape[0] // 2
        if not self.square:
            self.copies = [
                remote(src, dst.at[f], snd.at[k - 1], rcv.at[k - 1], (s, lax.rem(f + k, n_f))) for k in range(1, n_f)
            ]
            return
        one = f + 1 - 2 * lax.rem(f, 2)
        two = f + 2 - 4 * (f // 2)
        low, high = pl.ds(0, rows), pl.ds(rows, rows)

        def send(i, source, owner, part, target):
            return remote(source, dst.at[owner, part], snd.at[i], rcv.at[i], (s, target))

        self.copies = [
            send(0, src.at[low], f, low, one),
            send(1, src.at[high], f, high, two),
            send(2, src.at[high], f, high, one),
            send(3, src.at[low], f, low, two),
        ]
        self.onward = [
            send(4, dst.at[one, low], one, low, two),
            send(5, dst.at[two, high], two, high, one),
        ]

    def start(self):
        for copy in self.copies:
            copy.start()

    def pass_on(self):
        if self.square:
            for copy, more in zip(self.copies, self.onward):
                copy.wait_recv()
                more.start()

    def finish(self):
        if not self.square:
            for copy in self.copies:
                copy.wait()
            return
        for copy in self.copies[:2]:
            copy.wait_send()
        for copy in self.copies[2:] + self.onward:
            copy.wait()


def fan_sems(n_f):
    count = 6 if n_f == 4 else n_f - 1
    return [pltpu.SemaphoreType.DMA((count,)), pltpu.SemaphoreType.DMA((count,))]


def gather_kernel(n_s, n_f, C, DI, tok, seg, w, tok_all, seg_all, w_all, edge, edge_own, b_tok, b_w, b_seg, snd, rcv, loc, t_snd, t_rcv):
    s, f = place()
    L = tok.shape[0]
    tail = w.shape[0] - 2 * DI
    right, left = lax.rem(s + 1, n_s), lax.rem(s + n_s - 1, n_s)
    parity = lax.rem(s, 2)
    plane = lax.rem(s // 2, 2)
    pair = s + 1 - 2 * parity
    across = s + 2 - 4 * plane
    peers = [lax.rem(f + k, n_f) for k in range(1, n_f)]
    meet([(right, f), (left, f), (across, f)] + [(s, p) for p in peers])
    count = [0]

    def go(src, dst, target):
        i = count[0]
        count[0] = i + 1
        copy = remote(src, dst, snd.at[i], rcv.at[i], target)
        copy.start()
        return copy

    def quarter(base, c, p):
        width = C // 4
        return pl.ds(pl.multiple_of(base + (2 * c + p) * width, 8), width)

    def side(base):
        width = tail // 2
        return pl.ds(pl.multiple_of(base + parity * width, 8), width)

    spots = (quarter(0, parity, plane), quarter(C, parity, plane))
    first = go(tok.at[pl.ds(L - EDGE, EDGE)], edge_own, (right, f))
    w_copies = []
    for p in peers:
        sources = (quarter(p * C, parity, plane), quarter(DI + p * C, parity, plane))
        w_copies.append([go(w.at[a], w_all.at[f, b], (s, p)) for a, b in zip(sources, spots)])
    tails = [go(w.at[side(2 * DI)], w_all.at[f, side(2 * C)], (s, p)) for p in peers]
    started = []
    for p in peers:
        started.append(go(seg, seg_all.at[f], (s, p)))
    fan = Fan(tok, tok_all, t_snd, t_rcv, n_f)
    fan.start()
    mine = [
        (tok, b_tok),
        (seg, b_seg),
        (w.at[pl.ds(pl.multiple_of(f * C, 8), C)], b_w.at[pl.ds(0, C)]),
        (w.at[pl.ds(pl.multiple_of(DI + f * C, 8), C)], b_w.at[pl.ds(C, C)]),
        (w.at[pl.ds(2 * DI, tail)], b_w.at[pl.ds(2 * C, tail)]),
    ]
    ins = [pltpu.make_async_copy(a, b, loc.at[i]) for i, (a, b) in enumerate(mine)]
    for c in ins:
        c.start()
    first.wait()
    edges = [go(edge_own, edge.at[f], (s, p)) for p in peers]
    outs = [pltpu.make_async_copy(edge_own, edge.at[f], loc.at[5])]
    outs[0].start()
    for c in ins:
        c.wait()
    for i, (a, b) in enumerate(((b_tok, tok_all.at[f]), (b_seg, seg_all.at[f]), (b_w, w_all.at[f]))):
        out = pltpu.make_async_copy(a, b, loc.at[6 + i])
        out.start()
        outs.append(out)
    sources = [lax.rem(f + n_f - (k + 1), n_f) for k in range(n_f - 1)]
    over, relays = [], []
    for source, copies in zip(sources, w_copies):
        for copy, spot in zip(copies, spots):
            copy.wait_recv()
            piece = w_all.at[source, spot]
            over.append(go(piece, piece, (across, f)))
            relays.append(go(piece, piece, (pair, f)))
    for source, copy in zip(sources, tails):
        copy.wait_recv()
        piece = w_all.at[source, side(2 * C)]
        relays.append(go(piece, piece, (pair, f)))
    fan.pass_on()
    for i, copy in enumerate(over):
        copy.wait_recv()
        base = C * (i % 2)
        piece = w_all.at[sources[i // 2], quarter(base, parity, 1 - plane)]
        relays.append(go(piece, piece, (pair, f)))
    for copy in relays:
        copy.wait()
    for copy in sum(w_copies, []) + tails + over:
        copy.wait_send()
    for copy in started + edges:
        copy.wait()
    fan.finish()
    for out in outs:
        out.wait()


def gather(tok, seg, w, C, DI, n_s, n_f):
    L, D = tok.shape
    R = w.shape[1]
    own = 2 * C + w.shape[0] - 2 * DI
    sems = 1 + 12 * (n_f - 1)
    outs = [
        jax.ShapeDtypeStruct((n_f, L, D), BF16),
        jax.ShapeDtypeStruct((n_f,) + seg.shape, seg.dtype),
        jax.ShapeDtypeStruct((n_f, own, R), BF16),
        jax.ShapeDtypeStruct((n_f, EDGE, D), BF16),
        jax.ShapeDtypeStruct((EDGE, D), BF16),
    ]
    return pl.pallas_call(
        functools.partial(gather_kernel, n_s, n_f, C, DI),
        name="gather",
        out_shape=outs,
        in_specs=[ANY] * 3,
        out_specs=[ANY] * 5,
        scratch_shapes=[
            pltpu.VMEM((L, D), BF16),
            pltpu.VMEM((own, R), BF16),
            pltpu.VMEM(seg.shape, seg.dtype),
            pltpu.SemaphoreType.DMA((sems,)),
            pltpu.SemaphoreType.DMA((sems,)),
            pltpu.SemaphoreType.DMA((9,)),
        ]
        + fan_sems(n_f),
        compiler_params=params(collective_id=0, has_side_effects=True),
    )(tok, seg, w)


def partner(n_f, k):
    f = lax.axis_index("fsdp")
    result = 0
    for level in range(n_f.bit_length() - 1):
        both = f // (1 << level) + (n_f - k) // (1 << level)
        result = result + lax.rem(both, 2) * (1 << level)
    return result


class RowExchange:
    def __init__(self, n_f, piece, land, keep_own, mate, total, sems, mine=None, loc=None):
        s, f = place()
        self.n_f, self.keep_own, self.mate, self.total = n_f, keep_own, mate, total
        core = lax.rem(s, 2)
        pair = s + 1 - 2 * core
        p_snd, p_rcv, snd, rcv = sems
        owners = [partner(n_f, k) for k in range(1, n_f + 1)]
        self.owners = owners
        self.near = [(pair, f)] + [(s, owner) for owner in owners[:-1]]
        self.gifts = [
            remote(piece(owner, 1 - core), mate.at[i], p_snd.at[i], p_rcv.at[i], (pair, f))
            for i, owner in enumerate(owners)
        ]
        self.kept = [piece(owner, core) for owner in owners]
        self.loads = []
        if mine is not None:
            self.loads = [pltpu.make_async_copy(a, mine.at[i], loc.at[i]) for i, a in enumerate(self.kept)]
            self.kept = [mine.at[i] for i in range(n_f)]
        self.copies = [
            remote(total.at[i], land(i), snd.at[i], rcv.at[i], (s, owner)) for i, owner in enumerate(owners[:-1])
        ]

    def begin(self):
        for copy in self.gifts + self.loads:
            copy.start()

    def push(self):
        for i, kept in enumerate(self.kept):
            if self.loads:
                self.loads[i].wait()
            self.gifts[i].wait_recv()
            value = half(kept[...].astype(F32) + self.mate[i].astype(F32))
            if i == self.n_f - 1:
                self.keep_own(value)
            else:
                self.total[i] = value
                self.copies[i].start()

    def arrived(self, i):
        if i < self.n_f - 1:
            self.copies[i].wait_recv()

    def end(self):
        for copy in self.gifts + self.copies:
            copy.wait_send()


def exchange_scratch(n_f, rows, R, load):
    dma = pltpu.SemaphoreType.DMA
    buffers = [pltpu.VMEM((n_f, rows, R), BF16), pltpu.VMEM((n_f - 1, rows, R), BF16)]
    sems = [dma((n_f,)), dma((n_f,)), dma((n_f - 1,)), dma((n_f - 1,))]
    return buffers + sems + ([pltpu.VMEM((n_f, rows, R), BF16), dma((n_f,))] if load else [])


class PairChain:
    def __init__(self, n_s, forward, state, through, mate, mate_through, came, sent, sems):
        s, f = place()
        core, chip, chips = lax.rem(s, 2), s // 2, n_s // 2
        pair = s + 1 - 2 * core
        target = lax.rem(s + 2, n_s) if forward else lax.rem(s + n_s - 2, n_s)
        other = lax.rem(s + n_s - 2, n_s) if forward else lax.rem(s + 2, n_s)
        self.near = [(pair, f), (target, f), (other, f)]
        self.master = core == (1 if forward else 0)
        self.first = chip == (0 if forward else chips - 1)
        self.last = chip == (chips - 1 if forward else 0)
        self.position = chip if forward else chips - 1 - chip
        self.state, self.through, self.mate, self.mate_through = state, through, mate, mate_through
        self.came, self.sent = came, sent
        count = state.shape[0]
        self.count = count
        mate_snd, mate_rcv, on_snd, in_rcv, fwd_snd = sems
        self.gift = [remote(state.at[q], mate.at[q], mate_snd.at[q], mate_rcv.at[q], (pair, f)) for q in range(count)]
        self.gift_through = remote(through, mate_through, mate_snd.at[count], mate_rcv.at[count], (pair, f))
        self.on = [remote(sent.at[q], came.at[q], on_snd.at[q], in_rcv.at[q], (target, f)) for q in range(count)]
        self.forward = [remote(came.at[q], came.at[q], fwd_snd.at[q], in_rcv.at[q], (pair, f)) for q in range(count)]

    def begin(self):
        @pl.when(jnp.logical_not(self.master))
        def _():
            self.gift_through.start()
            for copy in self.gift:
                copy.start()

    def joined(self, q):
        return self.mate[q].astype(F32) + self.came[q].astype(F32) * self.mate_through[q, 0:1, :]

    def send_on(self, q):
        total = self.state_of(q).astype(F32) + self.joined(q) * self.through_of(q)
        self.sent[q] = half(total)
        self.on[q].start()

    def state_of(self, q):
        return self.state[q]

    def through_of(self, q):
        return self.through[q, 0:1, :]

    def mate_ready(self, q):
        if q == 0:
            self.gift_through.wait_recv()
        self.gift[q].wait_recv()

    def early(self, q):
        @pl.when(self.first)
        def _():
            self.came[q] = jnp.zeros_like(self.came[q])

        @pl.when(jnp.logical_and(self.master, self.first))
        def _():
            self.mate_ready(q)
            self.send_on(q)

    def late(self, q):
        @pl.when(jnp.logical_not(self.first))
        def _():
            self.on[q].wait_recv()

        @pl.when(jnp.logical_and(self.master, jnp.logical_not(self.first)))
        def _():
            self.forward[q].start()
            self.mate_ready(q)

            @pl.when(jnp.logical_not(self.last))
            def _():
                self.send_on(q)

    def write_entering(self, q, out):
        @pl.when(self.master)
        def _():
            out[...] = half(self.joined(q))

        @pl.when(jnp.logical_not(self.master))
        def _():
            out[...] = self.came[q]

    def end(self):
        @pl.when(jnp.logical_not(self.master))
        def _():
            self.gift_through.wait_send()
            for copy in self.gift:
                copy.wait_send()

        @pl.when(jnp.logical_and(self.master, jnp.logical_not(self.last)))
        def _():
            for copy in self.on:
                copy.wait_send()

        @pl.when(jnp.logical_and(self.master, jnp.logical_not(self.first)))
        def _():
            for copy in self.forward:
                copy.wait_send()


def chain_scratch(n_f, N, C):
    dma = pltpu.SemaphoreType.DMA
    return [
        pltpu.VMEM((n_f, N, C), BF16),
        pltpu.VMEM((n_f, 8, C), F32),
        pltpu.VMEM((n_f, N, C), BF16),
        pltpu.VMEM((n_f, N, C), BF16),
        dma((n_f + 1,)), dma((n_f + 1,)), dma((n_f,)), dma((n_f,)), dma((n_f,)),
    ]


def slab_steps(n_f, product, sent, got, own, snd, rcv):
    s, f = place()

    def copy(k):
        return remote(sent.at[k - 1], got.at[k - 1], snd.at[k - 1], rcv.at[k - 1], (s, partner(n_f, k)))

    def step(k, carry=0):
        slab = product(partner(n_f, k))

        @pl.when(k < n_f)
        def _():
            sent[k - 1] = half(slab)
            copy(k).start()

        @pl.when(k == n_f)
        def _():
            own[...] = slab

        return carry

    def finish():
        total = own[...]
        for k in range(1, n_f):
            copy(k).wait()
            total = total + got[k - 1].astype(F32)
        return total

    return [(s, lax.rem(f + k, n_f)) for k in range(1, n_f)], step, finish


def slab_scratch(n_f, L, D):
    return [
        pltpu.VMEM((n_f - 1, L, D), BF16),
        pltpu.VMEM((n_f - 1, L, D), BF16),
        pltpu.VMEM((L, D), F32),
        pltpu.SemaphoreType.DMA((n_f - 1,)),
        pltpu.SemaphoreType.DMA((n_f - 1,)),
    ]


def out_kernel(
    n_s, n_f, state, through, ngate_t, dz_t, normed, cot,
    result, g_out, g_z,
    b_ngt, b_dzt, b_norm, b_cot, own_z, loc,
    mate, mate_through, came, gone, m_snd, m_rcv, o_snd, i_rcv, f_snd,
    x_mate, x_total, x_psnd, x_prcv, x_snd, x_rcv,
):
    chain = PairChain(n_s, False, state, through, mate, mate_through, came, gone, (m_snd, m_rcv, o_snd, i_rcv, f_snd))
    loads = [
        pltpu.make_async_copy(a, b, loc.at[i])
        for i, (a, b) in enumerate(
            ((ngate_t, b_ngt), (cot, b_cot), (dz_t, b_dzt), (normed, b_norm))
        )
    ]
    for load in loads:
        load.start()

    s, f = place()
    C = g_out.shape[0]
    width = C // 2
    keep = pl.ds(pl.multiple_of(lax.rem(s, 2) * width, 16), width)
    give = pl.ds(pl.multiple_of((1 - lax.rem(s, 2)) * width, 16), width)

    def piece(owner, side):
        return own_z.at[owner, pl.ds(pl.multiple_of(side * width, 16), width)]

    def keep_own(value):
        g_z[f, keep, :] = value

    swap = RowExchange(
        n_f, piece, lambda i: g_z.at[f, keep], keep_own, x_mate, x_total, (x_psnd, x_prcv, x_snd, x_rcv)
    )
    meet(chain.near[1:] + swap.near)
    chain.begin()
    for q in range(chain.count):
        chain.early(q)
    for load in loads:
        load.wait()
    rows = C // n_f

    def z_rows(i, carry):
        mine = pl.ds(pl.multiple_of(i * rows, 16), rows)
        for j in range(n_f):
            acc = mm(b_dzt[0, mine, :], b_norm[0, j], NN)
            for q in range(1, n_f):
                acc = acc + mm(b_dzt[q, mine, :], b_norm[q, j], NN)
            own_z[j, mine, :] = half(acc)
        return carry

    def out_rows(i, carry):
        mine = pl.ds(pl.multiple_of(i * rows, 16), rows)
        acc = mm(b_ngt[0, mine, :], b_cot[0], NN)
        for q in range(1, n_f):
            acc = acc + mm(b_ngt[q, mine, :], b_cot[q], NN)
        g_out[mine, :] = half(acc)
        return carry

    lax.fori_loop(0, n_f, z_rows, 0)
    swap.begin()
    lax.fori_loop(0, n_f, out_rows, 0)
    for j in range(n_f):
        g_z[j, give, :] = jnp.zeros((width, g_z.shape[2]), BF16)
    swap.push()
    for q in range(chain.count):
        chain.late(q)
        chain.write_entering(q, result.at[q])
    for i in range(n_f):
        swap.arrived(i)
    swap.end()
    chain.end()


def chain_and_products(states, through, ngate_t, dz_t, normed, cot, n_s, n_f):
    D = cot.shape[-1]
    n, N_, C = states.shape
    R = normed.shape[-1]
    return pl.pallas_call(
        functools.partial(out_kernel, n_s, n_f),
        name="chain_back",
        out_shape=[
            jax.ShapeDtypeStruct(states.shape, BF16),
            jax.ShapeDtypeStruct((C, D), BF16),
            jax.ShapeDtypeStruct((n_f, C, R), BF16),
        ],
        in_specs=[VMEM] * 2 + [ANY] * 4,
        out_specs=[VMEM] * 3,
        scratch_shapes=[
            pltpu.VMEM(a.shape, BF16) for a in (ngate_t, dz_t, normed, cot)
        ]
        + [pltpu.VMEM((n_f, C, R), BF16), pltpu.SemaphoreType.DMA((4,))]
        + chain_scratch(n_f, N_, C)
        + exchange_scratch(n_f, C // 2, R, False),
        compiler_params=params(collective_id=2, has_side_effects=True),
    )(states, through, ngate_t, dz_t, normed, cot)


class LineSum:
    def __init__(self, n_s, own, final, inward, across, outgoing, sems):
        s, f = place()
        chips, chip, core = n_s // 2, s // 2, lax.rem(s, 2)
        pair = s + 1 - 2 * core
        low = chip < chips // 2
        way = jnp.where(low, 2, -2)
        self.middle = jnp.logical_or(chip == chips // 2 - 1, chip == chips // 2)
        self.edge = jnp.logical_or(chip == 0, chip == chips - 1)
        inner = s + way
        outer = lax.rem(s - way + n_s, n_s)
        self.near = [(pair, f), (inner, f), (outer, f)]
        self.own, self.final, self.inward, self.across, self.outgoing = own, final, inward, across, outgoing
        self.count = len(own)
        i_snd, i_rcv, x_rcv, o_snd, o_rcv, p_snd, p_rcv = sems
        spread = range(self.count)
        self.to_inner = [remote(outgoing[p], inward[p], i_snd.at[p], i_rcv.at[p], (inner, f)) for p in spread]
        self.to_other = [remote(outgoing[p], across[p], i_snd.at[p], x_rcv.at[p], (inner, f)) for p in spread]
        self.to_outer = [remote(final[p], final[p], o_snd.at[p], o_rcv.at[p], (outer, f)) for p in spread]
        self.to_pair = [remote(final[p], final[p], p_snd.at[p], p_rcv.at[p], (pair, f)) for p in spread]

    def inwards(self, p):
        @pl.when(self.edge)
        def _():
            self.outgoing[p][...] = self.own[p][...]

        @pl.when(jnp.logical_not(self.edge))
        def _():
            self.to_inner[p].wait_recv()
            total = self.own[p][...].astype(F32) + self.inward[p][...].astype(F32)
            self.outgoing[p][...] = half(total)

        @pl.when(self.middle)
        def _():
            self.to_other[p].start()

        @pl.when(jnp.logical_not(self.middle))
        def _():
            self.to_inner[p].start()

    def outwards(self, p):
        @pl.when(self.middle)
        def _():
            self.to_other[p].wait_recv()
            total = self.outgoing[p][...].astype(F32) + self.across[p][...].astype(F32)
            self.final[p][...] = half(total)

        @pl.when(jnp.logical_not(self.middle))
        def _():
            self.to_outer[p].wait_recv()

        @pl.when(jnp.logical_not(self.edge))
        def _():
            self.to_outer[p].start()

        self.to_pair[p].start()

    def run(self, ready):
        @pl.when(self.middle)
        def _():
            for p in range(self.count):
                ready(p)
                self.inwards(p)
                if p:
                    self.outwards(p - 1)
            self.outwards(self.count - 1)

        @pl.when(jnp.logical_not(self.middle))
        def _():
            for p in range(self.count):
                ready(p)
                self.inwards(p)
            for p in range(self.count):
                self.outwards(p)

    def end(self):
        for p in range(self.count):
            self.to_pair[p].wait()
            self.to_inner[p].wait_send()

        @pl.when(jnp.logical_not(self.edge))
        def _():
            for p in range(self.count):
                self.to_outer[p].wait_send()


def finish_kernel(
    n_s, n_f, data, dz, dx, dbd, w, tok, cot, gain,
    grad, g_pre, g_x, g_b,
    b_dz, b_dx, b_dbd, b_w, loc,
    xm, xt, xps, xpr, xs, xr, xo, xl,
    bm, bt, bps, bpr, bs, br, bo, bl,
    x_came, b_came, b_sum, x_in, x_ac, x_go, b_in, b_ac, b_go,
    i_snd, i_rcv, a_rcv, o_snd, o_rcv, p_snd, p_rcv,
    sent, got, own, snd, rcv,
):
    s, f = place()
    C = dz.shape[2]
    core = lax.rem(s, 2)
    wide, narrow = C // 2, (data.shape[1] - C) // 2
    loads = [
        pltpu.make_async_copy(a, b, loc.at[i])
        for i, (a, b) in enumerate(((w, b_w), (dz, b_dz), (dx, b_dx), (dbd, b_dbd)))
    ]

    def x_piece(owner, side):
        return data.at[owner, pl.ds(pl.multiple_of(side * wide, 8), wide)]

    def b_piece(owner, side):
        return data.at[owner, pl.ds(pl.multiple_of(C + side * narrow, 8), narrow)]

    def x_own(value):
        x_came[n_f - 1] = value

    def b_own(value):
        b_came[n_f - 1] = value

    x_swap = RowExchange(n_f, x_piece, lambda i: x_came.at[i], x_own, xm, xt, (xps, xpr, xs, xr), xo, xl)
    b_swap = RowExchange(n_f, b_piece, lambda i: b_came.at[i], b_own, bm, bt, (bps, bpr, bs, br), bo, bl)

    def product(q):
        blocks = []
        for j in range(n_f):
            block = mm(b_dz[q], b_w[j, 0:C, :], NN) + mm(b_dx[q], b_w[j, C : 2 * C, :], NN)
            blocks.append(block + mm(b_dbd[q], b_w[j, 2 * C :, :], NN))
        return jnp.concatenate(blocks, 1)

    peers, step, finish = slab_steps(n_f, product, sent, got, own, snd, rcv)
    order = [n_f - 1] + list(range(n_f - 1))
    part = wide // 2
    mine, final, inward, across, outgoing, slot = [], [], [], [], [], []
    for i in order:
        for h in range(2):
            rows = pl.ds(h * part, part)
            place_at = pl.ds(pl.multiple_of(core * wide + h * part, 8), part)
            mine.append(x_came.at[i, rows])
            final.append(g_x.at[x_swap.owners[i], place_at])
            inward.append(x_in.at[i, rows])
            across.append(x_ac.at[i, rows])
            outgoing.append(x_go.at[i, rows])
            slot.append(i)
    b_rows = pl.ds(pl.multiple_of(core * narrow, 8), narrow)
    mine.append(b_sum)
    final.append(g_b.at[b_rows])
    inward.append(b_in)
    across.append(b_ac)
    outgoing.append(b_go)
    line = LineSum(n_s, mine, final, inward, across, outgoing, (i_snd, i_rcv, a_rcv, o_snd, o_rcv, p_snd, p_rcv))

    def ready(p):
        if p == len(slot):
            value = b_came[n_f - 1].astype(F32)
            for i in range(n_f - 1):
                b_swap.arrived(i)
                value = value + b_came[i].astype(F32)
            b_sum[...] = half(value)
        elif p % 2 == 0:
            x_swap.arrived(slot[p])

    meet(line.near + peers)
    x_swap.begin()
    b_swap.begin()
    for load in loads:
        load.start()
    x_swap.push()
    b_swap.push()
    for load in loads:
        load.wait()
    lax.fori_loop(1, n_f + 1, step, 0)
    line.run(ready)
    tokf = tok[...].astype(F32)
    inv = lax.rsqrt(jnp.mean(tokf * tokf, 1, keepdims=True) + EPSILON)
    scaled = tokf * inv
    gn = finish()
    g_pre[...] = jnp.broadcast_to(jnp.sum(gn * scaled, 0, keepdims=True), g_pre.shape)
    weighted = gn * gain[...]
    grad[...] = half(
        cot[...].astype(F32) + inv * (weighted - scaled * jnp.mean(weighted * scaled, 1, keepdims=True))
    )
    line.end()
    x_swap.end()
    b_swap.end()


def finish_all(data, dz, dx, dbd, w, tok, cot, gain, n_s, n_f):
    L, D = tok.shape
    n, C, R = w.shape[0], dz.shape[2], w.shape[2]
    wide, narrow = C // 2, (data.shape[1] - C) // 2
    pieces = 2 * n_f + 1
    dma = pltpu.SemaphoreType.DMA
    x_buf, b_buf = pltpu.VMEM((n_f, wide, R), BF16), pltpu.VMEM((narrow, R), BF16)
    return pl.pallas_call(
        functools.partial(finish_kernel, n_s, n_f),
        name="finish",
        out_shape=[
            jax.ShapeDtypeStruct((L, D), BF16),
            jax.ShapeDtypeStruct((8, D), F32),
            jax.ShapeDtypeStruct((n_f, C, R), BF16),
            jax.ShapeDtypeStruct((2 * narrow, R), BF16),
        ],
        in_specs=[ANY] * 5 + [VMEM] * 3,
        out_specs=[VMEM] * 4,
        scratch_shapes=[pltpu.VMEM(a.shape, BF16) for a in (dz, dx, dbd, w)]
        + [dma((4,))]
        + exchange_scratch(n_f, wide, R, True)
        + exchange_scratch(n_f, narrow, R, True)
        + [x_buf, pltpu.VMEM((n_f, narrow, R), BF16), b_buf, x_buf, x_buf, x_buf, b_buf, b_buf, b_buf]
        + [dma((pieces,))] * 7
        + slab_scratch(n_f, L, D),
        compiler_params=params(collective_id=4, has_side_effects=True),
    )(data, dz, dx, dbd, w, tok, cot, gain)


def small_rows(C, D, pair):
    return 8 * C // LANES, 8, 8 * pair // LANES, -(-(D // LANES) // 8) * 8


def small_kernel(n_s, n_f, g_x, g_gain, g_h, g_b, g_pre, everything, buf, got, snd, rcv, f_snd, f_rcv):
    s, f = place()
    C, D, pair = g_x.shape[1], g_pre.shape[1], g_b.shape[1]
    counts = small_rows(C, D, pair)
    levels = n_s.bit_length() - 1

    def flip(k):
        bit = 1 << k
        return s + bit - 2 * bit * lax.rem(s // bit, 2)

    meet([(flip(k), f) for k in range(levels)] + [(s, lax.rem(f + k, n_f)) for k in range(1, n_f)])
    row = lax.broadcasted_iota(jnp.int32, (8, LANES), 0)
    for j in range(C // LANES):
        lanes = slice(j * LANES, (j + 1) * LANES)
        buf[0, 8 * j : 8 * j + 8, :] = jnp.where(row == TAPS + 1, g_gain[:, lanes], g_x[:, lanes])
    at = counts[0]
    buf[0, at : at + 8, :] = g_h[...]
    at += 8
    for j in range(pair // LANES):
        buf[0, at + 8 * j : at + 8 * j + 8, :] = g_b[:, j * LANES : (j + 1) * LANES]
    at += counts[2]
    for j in range(D // LANES):
        buf[0, at + j : at + j + 1, :] = g_pre[0:1, j * LANES : (j + 1) * LANES]
    for j in range(D // LANES, counts[3]):
        buf[0, at + j : at + j + 1, :] = jnp.zeros((1, LANES), F32)
    for k in range(levels):
        copy = remote(buf.at[k], got.at[k], snd.at[k], rcv.at[k], (flip(k), f))
        copy.start()
        copy.wait()
        buf[k + 1] = buf[k] + got[k]
    everything[f] = buf[levels]
    copies = []
    for k in range(1, n_f):
        target = (s, lax.rem(f + k, n_f))
        copy = remote(buf.at[levels], everything.at[f], f_snd.at[k - 1], f_rcv.at[k - 1], target)
        copy.start()
        copies.append(copy)
    for copy in copies:
        copy.wait()


def spread_small_kernel(n_f, DI, D, everything, conv_w, conv_b, gain, pre, heads):
    pair = conv_w.shape[1] - DI
    C = DI // n_f
    counts = small_rows(C, D, pair)
    for f in range(n_f):
        for j in range(C // LANES):
            lanes = slice(f * C + j * LANES, f * C + (j + 1) * LANES)
            conv_w[:, lanes] = everything[f, 8 * j : 8 * j + TAPS, :]
            conv_b[:, lanes] = everything[f, 8 * j + TAPS : 8 * j + TAPS + 1, :]
            gain[:, lanes] = everything[f, 8 * j + TAPS + 1 : 8 * j + TAPS + 2, :]
        heads[f] = everything[f, counts[0] : counts[0] + 8, :]
    at = counts[0] + 8
    both = everything[0, at:, :]
    for f in range(1, n_f):
        both = both + everything[f, at:, :]
    for j in range(pair // LANES):
        lanes = slice(DI + j * LANES, DI + (j + 1) * LANES)
        conv_w[:, lanes] = both[8 * j : 8 * j + TAPS]
        conv_b[:, lanes] = both[8 * j + TAPS : 8 * j + TAPS + 1]
    for j in range(D // LANES):
        pre[:, j * LANES : (j + 1) * LANES] = both[counts[2] + j : counts[2] + j + 1]


def small_sums(g_x, g_gain, g_h, g_b, g_pre, n_s, n_f):
    C, D, pair = g_x.shape[1], g_pre.shape[1], g_b.shape[1]
    rows = sum(small_rows(C, D, pair))
    levels = n_s.bit_length() - 1
    DI = C * n_f
    everything = pl.pallas_call(
        functools.partial(small_kernel, n_s, n_f),
        name="small",
        out_shape=jax.ShapeDtypeStruct((n_f, rows, LANES), F32),
        in_specs=[VMEM] * 5,
        out_specs=VMEM,
        scratch_shapes=[
            pltpu.VMEM((levels + 1, rows, LANES), F32),
            pltpu.VMEM((levels, rows, LANES), F32),
            pltpu.SemaphoreType.DMA((levels,)),
            pltpu.SemaphoreType.DMA((levels,)),
            pltpu.SemaphoreType.DMA((n_f - 1,)),
            pltpu.SemaphoreType.DMA((n_f - 1,)),
        ],
        compiler_params=params(collective_id=5, has_side_effects=True),
    )(g_x, g_gain, g_h, g_b, g_pre)
    return pl.pallas_call(
        functools.partial(spread_small_kernel, n_f, DI, D),
        name="spread_small",
        out_shape=[
            jax.ShapeDtypeStruct((TAPS, DI + pair), F32),
            jax.ShapeDtypeStruct((1, DI + pair), F32),
            jax.ShapeDtypeStruct((1, DI), F32),
            jax.ShapeDtypeStruct((1, D), F32),
            jax.ShapeDtypeStruct((n_f, 8, LANES), F32),
        ],
        in_specs=[VMEM],
        out_specs=[VMEM] * 5,
    )(everything)


def fill(scratch, halo, raw):
    length = raw.shape[0]
    scratch[0:EDGE, :] = halo.astype(F32)
    scratch[EDGE : EDGE + length, :] = raw.astype(F32)


def conv(scratch, length, kernel, bias, cols):
    pre = bias[...] + kernel[HALO : HALO + 1, :] * scratch[EDGE : EDGE + length, :]
    for k in range(HALO):
        start = EDGE - HALO + k
        pre = pre + kernel[k : k + 1, :] * (scratch[start : start + length, :] * cols[:, k : k + 1])
    return pre


def silu(value):
    return value * jax.nn.sigmoid(value)


def head_rows(values, pick):
    a = half(values)
    rest = values - a.astype(F32)
    b = half(rest)
    c = half(rest - b.astype(F32))
    rows = mm(a, pick, NN) + mm(b, pick, NN) + mm(c, pick, NN)
    used = jnp.sum(pick.astype(F32), 0, keepdims=True)
    return rows[0:1, :] + 100.0 * (used - 1.0), jnp.exp(rows[1:2, :]), rows[2:3, :]


def marks_of(seg, before, s):
    L = seg.shape[1]
    before = jnp.where(s > 0, before, -1)
    both = jnp.concatenate([before, seg], 1)
    rows = [(both[:, L - k : 2 * L - k] == seg).astype(F32) for k in range(HALO, 0, -1)]
    rows.append((seg == seg[:, L - 1 : L]).astype(F32))
    rows.append((seg == before[:, L - 1 : L]).astype(F32))
    rows.append(seg.astype(F32))
    return jnp.concatenate(rows + [jnp.zeros((LANES - len(rows), L), F32)], 0)


def block_rows(L):
    return min(L, 128)


def live_rows(cols, seg_row, r, rows, width):
    row = lax.broadcasted_iota(jnp.int32, (rows, width), 0) + r * rows
    col = lax.broadcasted_iota(jnp.int32, (rows, width), 1)
    same = cols[r * rows : (r + 1) * rows, 5:6] == seg_row[0:1, 0:width]
    return (row >= col) & same


def front_kernel(
    tok, edge, w, pre_gain, seg, before, pick, hv, kw_x, kb_x, kw_b, kb_b, cot,
    cot_all, z, x, x_halo, b, b_halo, d, normed, cols, seg_row, state, through, pre_x, xd, pre_b, bc, cum, cum_row, plain, s_x, s_b, c_snd, c_rcv, c_own,
):
    L, C = x.shape
    n_f, _, R = w.shape
    at = pl.program_id(0)
    fan = Fan(cot, cot_all, c_snd, c_rcv, n_f)
    s, f = place()
    own = pltpu.make_async_copy(cot, cot_all.at[f], c_own)

    @pl.when(at == 0)
    def _():
        meet([(s, lax.rem(f + k, n_f)) for k in range(1, n_f)])
        fan.start()
        own.start()

    @pl.when(at == min(2, n_f - 1))
    def _():
        fan.pass_on()

    tokf = jnp.concatenate([edge[...], tok[...]], 0).astype(F32)
    inv = lax.rsqrt(jnp.mean(tokf * tokf, 1, keepdims=True) + EPSILON)
    n = half(tokf * inv * pre_gain[...])
    acc = mm(n[:, 0:R], w[0], NT)
    normed[0] = n[EDGE:, 0:R]
    for j in range(1, n_f):
        acc = acc + mm(n[:, j * R : (j + 1) * R], w[j], NT)
        normed[j] = n[EDGE:, j * R : (j + 1) * R]
    p = half(acc)
    z[...] = p[EDGE:, 0:C]
    x[...] = p[EDGE:, C : 2 * C]
    b[...] = p[EDGE:, 2 * C : 2 * C + 2 * N]
    inside = s > 0
    pe = p[0:EDGE, :].astype(F32)
    pe = half(jnp.where(inside, pe, 0.0))
    x_halo[...] = pe[:, C : 2 * C]
    b_halo[...] = pe[:, 2 * C : 2 * C + 2 * N]
    d[...] = half(mm(p[EDGE:, 2 * C + 2 * N :], pick[...], NN))

    table = head_table(C)
    m = marks_of(seg[...], before[...], s)
    seg_row[...] = jnp.broadcast_to(m[5:6, :], seg_row.shape)
    c = jnp.transpose(m)
    cols[...] = c
    fill(s_x, x_halo[...], x[...])
    fill(s_b, b_halo[...], b[...])
    px = conv(s_x, L, kw_x, kb_x, c)
    pb = conv(s_b, L, kw_b, kb_b, c)
    pre_x[...] = px
    pre_b[...] = pb
    bc[...] = half(silu(pb))
    bias, decay, _ = head_rows(hv[...], pick[...])
    step = softplus(d[...].astype(F32) + bias)
    rate = -step * decay
    total = running_sum(rate, True)
    cum[...] = total
    cum_row[...] = jnp.transpose(total)[0 : cum_row.shape[0], :]
    last = total[L - 1 : L, :]
    to_end = jnp.exp(last - total) * c[:, 3:4]
    entry_last = jnp.exp(last) * c[L - 1 : L, 4:5]
    through[...] = split_dot(jnp.broadcast_to(entry_last, (8, LANES)), table, NN)
    xdv = split_dot(step, table, NN) * silu(px)
    xd[...] = half(xdv)
    wx = half(split_dot(to_end, table, NN) * xdv)
    state[...] = half(mm(bc[:, 0:N], wx, TN))
    rows = block_rows(L)
    for r in range(L // rows):
        width = (r + 1) * rows
        mine = slice(r * rows, (r + 1) * rows)
        scores = jnp.where(
            live_rows(cols, seg_row, r, rows, width), mm(bc[mine, N : 2 * N], bc[0:width, 0:N], NT), 0.0
        )
        for h in range(0, C // P_SIZE, 2):
            pieces = []
            for i in (h, h + 1):
                gap = jnp.minimum(cum[mine, i : i + 1] - cum_row[i : i + 1, 0:width], 0.0)
                pieces.append(mm(scores * jnp.exp(gap), xd[0:width, i * P_SIZE : (i + 1) * P_SIZE], NN))
            plain[mine, h * P_SIZE : (h + 2) * P_SIZE] = jnp.concatenate(pieces, 1)

    @pl.when(at == n_f - 1)
    def _():
        own.wait()
        fan.finish()


def mix_kernel(
    n_s, n_f, cot, w_out, pre_x, inside, bc, cum, cols, state, through, z, gain, pick, hv,
    gg, enter, plain, mixed, total,
    mate, mate_through, came, gone, m_snd, m_rcv, o_snd, i_rcv, f_snd, part, got, t_snd, t_rcv,
):
    L, C = inside.shape
    table = head_table(C)
    step = pl.program_id(0)
    chain = PairChain(n_s, True, state, through, mate, mate_through, came, gone, (m_snd, m_rcv, o_snd, i_rcv, f_snd))
    s, f = place()

    def share(k, q):
        return remote(
            part.at[q], got.at[k - 1, q], t_snd.at[k - 1, q], t_rcv.at[k - 1, q], (s, lax.rem(f + k, n_f))
        )

    @pl.when(step == 0)
    def _():
        meet(chain.near + [(s, lax.rem(f + k, n_f)) for k in range(1, n_f)])
        chain.begin()

    for q in range(n_f):

        @pl.when(step == q)
        def _():
            chain.early(q)

    g = half(mm(cot[...], w_out[...], NT))
    gg[...] = g
    skip = head_rows(hv[...], pick[...])[2]
    skip = split_dot(jnp.broadcast_to(skip, (8, LANES)), table, NN)[0:1, :]
    entry = split_dot(jnp.exp(cum[...]) * cols[:, 4:5], table, NN)

    for q in range(n_f):

        @pl.when(step == q)
        def _():
            chain.late(q)
            chain.write_entering(q, enter)

    y = inside[...] + mm(bc[:, N : 2 * N], enter[...], NN) * entry
    plain[...] = y
    m = half(y + skip * silu(pre_x[...]))
    mixed[...] = m
    gated = m.astype(F32) * silu(z[...].astype(F32))
    sg = g.astype(F32) * gain[...]
    one = jnp.sum(gated * gated, 1, keepdims=True)
    two = jnp.sum(sg * gated, 1, keepdims=True)
    lane = lax.broadcasted_iota(jnp.int32, (L, LANES), 1)
    both = jnp.where(lane == 0, one, jnp.where(lane == 1, two, 0.0))
    part[step] = jnp.transpose(both)[0:8, :]
    for k in range(1, n_f):
        share(k, step).start()

    @pl.when(step == n_f - 1)
    def _():
        for q in range(n_f):
            value = part[q]
            for k in range(1, n_f):
                share(k, q).wait()
                value = value + got[k - 1, q]
            total[q] = value
        chain.end()


def gate_kernel(DI, mixed, z, gg, gain, total, cum, cols, bc, ngate, dz, dy, d_enter, ngate_t, dz_t, d_gain):
    L, C = mixed.shape
    table = head_table(C)
    sums = jnp.transpose(jnp.concatenate([total[...], jnp.zeros((LANES - 8, L), F32)], 0))
    inv = lax.rsqrt(sums[:, 0:1] / DI + EPSILON)
    inner = inv * (sums[:, 1:2] / DI)
    y = mixed[...].astype(F32)
    zf = z[...].astype(F32)
    sig = jax.nn.sigmoid(zf)
    gz = zf * sig
    unit = y * gz * inv
    g = gg[...].astype(F32)
    ng = half(unit * gain[...])
    ngate[...] = ng
    ngate_t[...] = jnp.transpose(ng)

    @pl.when(pl.program_id(0) == 0)
    def _():
        d_gain[...] = jnp.zeros_like(d_gain)

    d_gain[...] += jnp.broadcast_to(jnp.sum(g * unit, 0, keepdims=True), d_gain.shape)
    grad = inv * (g * gain[...] - unit * inner)
    d = half(grad * gz)
    dy[...] = d
    d_z = half(grad * y * sig * (1.0 + zf * (1.0 - sig)))
    dz[...] = d_z
    dz_t[...] = jnp.transpose(d_z)
    entry = jnp.exp(cum[...]) * cols[:, 4:5]
    edy = half(split_dot(entry, table, NN) * d.astype(F32))
    d_enter[...] = half(mm(bc[:, N : 2 * N], edy, TN))


def silu_grad(pre, sigma):
    return sigma * (1.0 + pre * (1.0 - sigma))


def conv_back(dpre, raw, halo, kernel, cols, s_raw, s_grad, grads):
    length = dpre.shape[0]
    fill(s_raw, halo, raw)
    grads[TAPS : TAPS + 1, :] += jnp.sum(dpre, 0, keepdims=True)
    grads[HALO : HALO + 1, :] += jnp.sum(dpre * s_raw[EDGE : EDGE + length, :], 0, keepdims=True)
    d_raw = kernel[HALO : HALO + 1, :] * dpre
    width = dpre.shape[1]
    d_halo = jnp.zeros((EDGE, width), F32)
    s_grad[0:EDGE, :] = jnp.zeros((EDGE, width), F32)
    s_grad[EDGE + length : EDGE + length + EDGE, :] = jnp.zeros((EDGE, width), F32)
    for k in range(HALO):
        masked = dpre * cols[:, k : k + 1]
        start = EDGE - HALO + k
        grads[k : k + 1, :] += jnp.sum(masked * s_raw[start : start + length, :], 0, keepdims=True)
        s_grad[EDGE : EDGE + length, :] = masked
        up = HALO - k
        d_raw = d_raw + kernel[k : k + 1, :] * s_grad[EDGE + up : EDGE + up + length, :]
        d_halo = d_halo + kernel[k : k + 1, :] * s_grad[up : up + EDGE, :]
    return d_raw, d_halo


def back_kernel(
    x, x_halo, b, b_halo, d, cols, seg_row, k_x, k_b, pick, hv, pre_x, xd, pre_b, bc, cum, cum_row, enter, grad, plain, dy,
    ngate, w_out, tok,
    dx, dbd, tail, halo, g_x, g_b, g_h, output,
    s_x, s_gx, s_b, s_gb, s_dxd, s_ds, sent, got, own, snd, rcv,
):
    L, C = xd.shape
    rows = block_rows(L)
    table = head_table(C)
    c = cols[...]
    cv = cum[...]
    bias, decay_rate, skip = head_rows(hv[...], pick[...])
    at = pl.program_id(0)
    n_f = ngate.shape[0]

    def product(q):
        return mm(ngate[q], w_out[...], NN)

    peers, step, finish = slab_steps(n_f, product, sent, got, own, snd, rcv)

    @pl.when(at == 0)
    def _():
        meet(peers)
        lax.fori_loop(1, n_f + 1, step, 0)

    @pl.when(at == 0)
    def _():
        g_x[...] = jnp.zeros_like(g_x)
        g_b[...] = jnp.zeros_like(g_b)
        g_h[...] = jnp.zeros_like(g_h)

    s_dxd[...] = jnp.zeros_like(s_dxd)
    s_ds[...] = jnp.zeros_like(s_ds)
    for r in range(L // rows):
        width = (r + 1) * rows
        mine = slice(r * rows, (r + 1) * rows)
        live = live_rows(cols, seg_row, r, rows, width)
        scores = jnp.where(live, mm(bc[mine, N : 2 * N], bc[0:width, 0:N], NT), 0.0)
        d_scores = jnp.zeros((rows, width), F32)
        for h in range(0, C // P_SIZE, 2):
            pieces = []
            for g in (h, h + 1):
                lanes = slice(g * P_SIZE, (g + 1) * P_SIZE)
                decay = jnp.exp(jnp.minimum(cum[mine, g : g + 1] - cum_row[g : g + 1, 0:width], 0.0))
                pieces.append(mm(scores * decay, dy[mine, lanes], TN))
                d_scores = d_scores + mm(dy[mine, lanes], xd[0:width, lanes], NT) * decay
            s_dxd[0:width, h * P_SIZE : (h + 2) * P_SIZE] += jnp.concatenate(pieces, 1)
        s_ds[mine, 0:width] = jnp.where(live, d_scores, 0.0)
    ds = half(s_ds[...])
    last = cv[L - 1 : L, :]
    to_end = split_dot(jnp.exp(last - cv) * c[:, 3:4], table, NN)
    entry = split_dot(jnp.exp(cv) * c[:, 4:5], table, NN)
    dyf = dy[...].astype(F32)
    xdf = xd[...].astype(F32)
    dwx = mm(bc[:, 0:N], grad[...], NN)
    wx = half(to_end * xdf)
    d_b = mm(wx, grad[...], NT) + mm(ds, bc[:, N : 2 * N], TN)
    d_c = mm(half(entry * dyf), enter[...], NT) + mm(ds, bc[:, 0:N], NN)
    u = split_dot(wx.astype(F32) * dwx, table, NT)
    dxd_in = s_dxd[...]
    dcum = split_dot(dyf * plain[...] - xdf * dxd_in, table, NT) - u
    carry = jnp.sum(enter[...].astype(F32) * grad[...].astype(F32), 0, keepdims=True)
    carry = split_dot(jnp.broadcast_to(carry, (8, C)), table, NT)[0:1, :]
    at_last = jnp.sum(u, 0, keepdims=True) + jnp.exp(last) * c[L - 1 : L, 4:5] * carry
    row = lax.broadcasted_iota(jnp.int32, (L, LANES), 0)
    dcum = dcum + jnp.where(row == L - 1, at_last, 0.0)
    drate = running_sum(dcum, False)
    px = pre_x[...]
    sig = jax.nn.sigmoid(px)
    xf = px * sig
    dxd = dxd_in + to_end * dwx
    raw_step = d[...].astype(F32) + bias
    size = softplus(raw_step)
    ddt = split_dot(xf * dxd, table, NT) - drate * decay_rate
    ddt_raw = ddt * jax.nn.sigmoid(raw_step)
    dbd[:, 2 * N :] = half(mm(ddt_raw, pick[...], NT))
    g_h[0:1, :] += jnp.sum(ddt_raw, 0, keepdims=True)
    g_h[1:2, :] += jnp.sum(drate * (-size * decay_rate), 0, keepdims=True)
    g_h[2:3, :] += split_dot(jnp.broadcast_to(jnp.sum(dyf * xf, 0, keepdims=True), (8, C)), table, NT)[0:1, :]
    skip = split_dot(jnp.broadcast_to(skip, (8, LANES)), table, NN)[0:1, :]
    d_x = split_dot(size, table, NN) * dxd + skip * dyf
    rx, hx = conv_back(d_x * silu_grad(px, sig), x[...], x_halo[...], k_x, c, s_x, s_gx, g_x)
    pb = pre_b[...]
    d_bc = jnp.concatenate([d_b, d_c], 1) * silu_grad(pb, jax.nn.sigmoid(pb))
    rb, hb = conv_back(d_bc, b[...], b_halo[...], k_b, c, s_b, s_gb, g_b)
    dx[...] = half(rx)
    dbd[:, 0 : 2 * N] = half(rb)
    tail[:, 0:C] = rx[L - EDGE : L, :]
    tail[:, C : C + 2 * N] = rb[L - EDGE : L, :]
    halo[:, 0:C] = half(hx)
    halo[:, C : C + 2 * N] = half(hb)

    @pl.when(at == n_f - 1)
    def _():
        output[...] = half(tok[...].astype(F32) + finish())


def weight_kernel(dx, dbd, normed, out, flipped):
    n_f, L, C = dx.shape

    @pl.when(pl.program_id(0) == 0)
    def _():
        for q in range(n_f):
            flipped[0:C, q * L : (q + 1) * L] = jnp.transpose(dx[q])
            flipped[C:, q * L : (q + 1) * L] = jnp.transpose(dbd[q])

    out[...] = half(mm(flipped[...], normed[...].reshape(n_f * L, normed.shape[-1]), NN))


def weight_grads(dx, dbd, normed):
    n_f, L, C = dx.shape
    B = dbd.shape[-1]
    W, R = C + B, normed.shape[-1]
    return pl.pallas_call(
        weight_kernel,
        name="weight_grads",
        grid_spec=pltpu.PrefetchScalarGridSpec(
            num_scalar_prefetch=0,
            grid=(n_f,),
            in_specs=[
                pl.BlockSpec((n_f, L, C), lambda k: (0, 0, 0)),
                pl.BlockSpec((n_f, L, B), lambda k: (0, 0, 0)),
                pl.BlockSpec((n_f, None, L, R), lambda k: (0, k, 0, 0)),
            ],
            out_specs=pl.BlockSpec((None, W, R), lambda k: (k, 0, 0)),
            scratch_shapes=[pltpu.VMEM((W, n_f * L), BF16)],
        ),
        out_shape=jax.ShapeDtypeStruct((n_f, W, R), BF16),
        compiler_params=params(dimension_semantics=("arbitrary",)),
        cost_estimate=pl.CostEstimate(flops=2 * n_f * L * W * R * n_f, bytes_accessed=4 * n_f * W * R, transcendentals=0),
    )(dx, dbd, normed)


def per(*shape, col=0):
    return pl.BlockSpec((None,) + shape, lambda q: (q, 0, col))


def fixed(*shape):
    return pl.BlockSpec(shape, lambda q: (0,) * len(shape))


def mine(*shape):
    return pl.BlockSpec(shape, lambda q: (0, lax.axis_index("fsdp")))


def shaped(*shape, dtype=F32):
    return jax.ShapeDtypeStruct(shape, dtype)


def shards(tokens, seg_ids, pre_gain, w_in, conv_weight, conv_bias, dt_bias, a_log, d_skip, norm_gain, w_out, cotangent):
    n_s = lax.axis_size("seq")
    n_f = lax.axis_size("fsdp")
    s = lax.axis_index("seq")
    f = lax.axis_index("fsdp")
    L, D = tokens.shape[1:]
    DI = norm_gain.shape[0]
    H = dt_bias.shape[0]
    Hl = H // n_f
    C = DI // n_f
    pair = conv_bias.shape[0] - DI
    T = n_f * L
    R = w_in.shape[0]
    W = 2 * C + pair + H
    HR = -(-Hl // 8) * 8

    pick = half((jnp.arange(H)[:, None] - f * Hl == jnp.arange(LANES)[None, :]) & (jnp.arange(LANES)[None, :] < Hl))
    hv = jnp.concatenate([dt_bias[None], a_log[None], d_skip[None], jnp.zeros((5, H), F32)], 0)
    gain = norm_gain[None]
    bias = conv_bias[None]
    pre = pre_gain[None]

    tok_all, seg_all, w_all, edge, _ = gather(tokens[0], seg_ids, w_in.T, C, DI, n_s, n_f)

    big, small, lane, st = per(L, C), per(L, pair), per(L, LANES), per(N, C)
    row8, halo_x, halo_b, hr = per(8, L), per(EDGE, C), per(EDGE, pair), per(HR, L)
    kw_x, kb_x = mine(TAPS, C), mine(1, C)
    kw_b = pl.BlockSpec((TAPS, pair), lambda q: (0, DI // pair))
    kb_b = pl.BlockSpec((1, pair), lambda q: (0, DI // pair))
    pick_spec, hv_spec = fixed(H, LANES), fixed(8, H)

    def call(body, name, ins, outs, shapes, flops, scratch=(), **more):
        return pl.pallas_call(
            body,
            name=name,
            grid_spec=pltpu.PrefetchScalarGridSpec(
                num_scalar_prefetch=0, grid=(n_f,), in_specs=ins, out_specs=outs, scratch_shapes=list(scratch)
            ),
            out_shape=shapes,
            compiler_params=params(dimension_semantics=("arbitrary",), **more),
            cost_estimate=pl.CostEstimate(flops=flops, bytes_accessed=20 * T * C, transcendentals=0),
        )

    cot_all, z, x, x_halo, b, b_halo, d, normed, cols, seg_row, state, through, pre_x, xd, pre_b, bc, cum, cum_row, inside = call(
        front_kernel,
        "front",
        [
            per(L, D), per(EDGE, D), fixed(n_f, W, R), fixed(1, D),
            pl.BlockSpec((None, 1, L), lambda q: (q, 0, lax.axis_index("seq"))),
            pl.BlockSpec((None, 1, L), lambda q: (q, 0, jnp.maximum(lax.axis_index("seq") - 1, 0))),
            pick_spec, hv_spec, kw_x, kb_x, kw_b, kb_b, VMEM,
        ],
        [
            ANY,
            big, big, halo_x, small, halo_b, lane, pl.BlockSpec((None, n_f, L, R), lambda q: (q, 0, 0, 0)), lane, row8,
            st, per(8, C), big, big, small, small, lane, hr, big,
        ],
        [
            shaped(n_f, L, D, dtype=BF16),
            shaped(n_f, L, C, dtype=BF16), shaped(n_f, L, C, dtype=BF16), shaped(n_f, EDGE, C, dtype=BF16),
            shaped(n_f, L, pair, dtype=BF16), shaped(n_f, EDGE, pair, dtype=BF16), shaped(n_f, L, LANES, dtype=BF16),
            shaped(n_f, n_f, L, R, dtype=BF16), shaped(n_f, L, LANES), shaped(n_f, 8, L),
            shaped(n_f, N, C, dtype=BF16), shaped(n_f, 8, C), shaped(n_f, L, C), shaped(n_f, L, C, dtype=BF16),
            shaped(n_f, L, pair), shaped(n_f, L, pair, dtype=BF16), shaped(n_f, L, LANES), shaped(n_f, HR, L),
            shaped(n_f, L, C),
        ],
        2 * T * D * W,
        [pltpu.VMEM((L + EDGE, C), F32), pltpu.VMEM((L + EDGE, pair), F32)] + fan_sems(n_f) + [pltpu.SemaphoreType.DMA],
        collective_id=3,
        has_side_effects=True,
    )(tok_all, edge, w_all, pre, seg_all, seg_all, pick, hv, conv_weight, bias, conv_weight, bias, cotangent[0])
    dma = pltpu.SemaphoreType.DMA
    ggate, enter, plain, mixed, total = call(
        functools.partial(mix_kernel, n_s, n_f),
        "mix",
        [
            per(L, D), fixed(C, D), big, big, small, lane, lane, fixed(n_f, N, C), fixed(n_f, 8, C), big,
            mine(1, C), pick_spec, hv_spec,
        ],
        [big, st, big, big, fixed(n_f, 8, L)],
        [
            shaped(n_f, L, C, dtype=BF16), shaped(n_f, N, C, dtype=BF16), shaped(n_f, L, C), shaped(n_f, L, C, dtype=BF16),
            shaped(n_f, 8, L),
        ],
        10 * T * D * C // 4,
        chain_scratch(n_f, N, C)
        + [
            pltpu.VMEM((n_f, 8, L), F32), pltpu.VMEM((n_f - 1, n_f, 8, L), F32), dma((n_f - 1, n_f)), dma((n_f - 1, n_f)),
        ],
        collective_id=1,
        has_side_effects=True,
    )(cot_all, w_out, pre_x, inside, bc, cum, cols, state, through, z, gain, pick, hv)
    turned = per(C, L)
    ngate, dz, dy, d_enter, ngate_t, dz_t, g_gain = call(
        functools.partial(gate_kernel, DI),
        "gate",
        [big, big, big, mine(1, C), row8, lane, lane, small],
        [big, big, big, st, turned, turned, fixed(8, C)],
        [shaped(n_f, L, C, dtype=BF16)] * 3
        + [shaped(n_f, N, C, dtype=BF16)]
        + [shaped(n_f, C, L, dtype=BF16)] * 2
        + [shaped(8, C)],
        T * D * C,
    )(mixed, z, ggate, gain, total, cum, cols, bc)
    grad, g_out, gz = chain_and_products(d_enter, through, ngate_t, dz_t, normed, cot_all, n_s, n_f)
    g_out, gz = lax.psum((g_out, gz), "seq")

    dx, dbd, tail, halo, g_x, g_b, g_h, output = call(
        back_kernel,
        "back",
        [
            big, halo_x, small, halo_b, lane, lane, row8, kw_x, kw_b, pick_spec, hv_spec,
            big, big, small, small, lane, hr, st, st, big, big, VMEM, VMEM, VMEM,
        ],
        [big, per(L, pair + H), per(EDGE, C + pair), per(EDGE, C + pair), fixed(8, C), fixed(8, pair), fixed(8, LANES), VMEM],
        [
            shaped(n_f, L, C, dtype=BF16), shaped(n_f, L, pair + H, dtype=BF16), shaped(n_f, EDGE, C + pair),
            shaped(n_f, EDGE, C + pair, dtype=BF16), shaped(8, C), shaped(8, pair), shaped(8, LANES),
            shaped(L, D, dtype=BF16),
        ],
        30 * T * D * C // 4,
        [
            pltpu.VMEM((L + EDGE, C), F32), pltpu.VMEM((L + 2 * EDGE, C), F32),
            pltpu.VMEM((L + EDGE, pair), F32), pltpu.VMEM((L + 2 * EDGE, pair), F32),
            pltpu.VMEM((L, C), F32), pltpu.VMEM((L, L), F32),
        ]
        + slab_scratch(n_f, L, D),
        collective_id=6,
        has_side_effects=True,
    )(x, x_halo, b, b_halo, d, cols, seg_row, conv_weight, conv_weight, pick, hv,
      pre_x, xd, pre_b, bc, cum, cum_row, enter, grad, plain, dy, ngate, w_out, tokens[0])
    got = lax.ppermute(halo, "seq", [(i + 1, i) for i in range(n_s - 1)])
    ends = half(tail + got.astype(F32))
    dx = lax.dynamic_update_slice(dx, ends[..., :C], (0, L - EDGE, 0))
    dbd = lax.dynamic_update_slice(dbd, ends[..., C:], (0, L - EDGE, 0))
    data = weight_grads(dx, dbd, normed)
    input_grad, g_pre, gx, gb = finish_all(data, dz, dx, dbd, w_all, tokens[0], cotangent[0], pre, n_s, n_f)
    g_in = jnp.concatenate([gz.reshape(DI, R), gx.reshape(DI, R), gb], 0).astype(F32).T
    conv_w, conv_b, g_gain, g_pre, g_h = small_sums(g_x, g_gain, g_h, g_b, g_pre, n_s, n_f)
    g_heads = [g_h[:, i, :Hl].reshape(H) for i in range(3)]
    return (output[None], input_grad[None], g_in, g_out.astype(F32), g_pre[0], conv_w, conv_b[0], *g_heads, g_gain[0])


def solution(mesh):
    seq, row, rep = P("fsdp", "seq", None), P("fsdp", None), P()
    in_specs = (seq, row, rep, row, rep, rep, rep, rep, rep, rep, row, seq)
    out_specs = (seq, seq, row, row) + (rep,) * 7
    return jax.shard_map(shards, mesh=mesh, in_specs=in_specs, out_specs=out_specs, check_vma=False)
```
